32 devices in a mesh: member: 2 (over y), slab: 4 (over z), chan: 2 (over x), mode: 2 (over core).
Axes of the slice: x: 2, y: 2, z: 4, core: 2. Of those that a mesh axis runs over, the one named last changes fastest.
Arguments:
- source_field: float32 [128, 1024, 1024], P(('member', 'chan'), 'slab', 'mode'), parts along dimension 0, may hold values from -6 to 6
- cotangent: float32 [128, 1024, 1024], P(('member', 'chan'), 'slab', 'mode'), parts along dimension 0, may hold values from -6 to 6
- spectral_weight: float32 [128, 64, 32, 2, 64], P(('member', 'chan'), None, 'mode', None, 'slab'), parts along dimension 0, may hold values from -12 to 12
- skip_gain: float32 [128], P(('member', 'chan')), parts along dimension 0, may hold values from 0.5 to 2
- channel_bias: float32 [128], P(('member', 'chan')), parts along dimension 0, may hold values from -0.5 to 0.5
- mode_limit: int32 [128, 2], P('member'), parts along dimension 0, may hold values from 16 to 32
- width_limit: int32 [128], P('member'), parts along dimension 0, may hold values from 32 to 64
Outputs:
- output: float32 [128, 1024, 1024], P(('member', 'chan'), 'slab', 'mode'), parts along dimension 0
- field_grad: float32 [128, 1024, 1024], P(('member', 'chan'), 'slab', 'mode'), parts along dimension 0
- spectral_grad: float32 [128, 64, 32, 2, 64], P(('member', 'chan'), None, 'mode', None, 'slab'), parts along dimension 0
- gate_grad: float32 [128], P(('member', 'chan')), parts along dimension 0
- bias_grad: float32 [128], P(('member', 'chan')), parts along dimension 0
The draws below stay inside these ranges and needn't reach their ends.
There are 2 independent parts, one for each index of `member`. The reference program is written for one: setup_inputs(seed, part) draws one part's arguments, and reference() takes and returns one part's arrays. A program takes and returns all parts, laid end to end along the dimension named above; each array names one. Nothing has to cross between parts.
Inputs may be any that keep to these rules, and one draw needn't show every extreme that they name: `mode_limit`: never more than 32. `width_limit`: never more than 64.
All inputs are finite; a program needn't handle non-finite values.
Results may differ from the reference program's by a relative error of at most 0.00018.
Values sent between devices are 32-bit elements; how exact they have to be, the bound alone decides.
No kernel may reach another device: no remote copies, remote signals or barrier semaphores. Data moves between devices by JAX's collectives and lax.ppermute only.
A program may use at most 192 MiB of HBM per device.

```python
import math
import jax
import jax.numpy as jnp
from jax import lax

C = 64
H = 1024
W = 1024
M = 32
KX = 64


def plant(values, stream_key, low, high):
    longest = values.shape.index(max(values.shape))
    spots = []
    for shift in (0, 1):
        where = [jax.random.randint(jax.random.fold_in(stream_key, axis), (), 0, length) for axis, length in enumerate(values.shape)]
        where[longest] = (where[longest] + shift) % values.shape[longest]
        spots.append(tuple(where))
    return values.at[spots[0]].set(low).at[spots[1]].set(high)


def levels(rng, shape, split, least, largest):
    factor_of = 1.0
    for dim, parts in split:
        steps = jax.random.uniform(jax.random.fold_in(jax.random.fold_in(rng, 6), dim), (parts,), jnp.float32, least / len(split), largest / len(split))
        factor_of = factor_of * jnp.repeat(jnp.exp(steps), shape[dim] // parts).reshape((-1,) + (1,) * (len(shape) - 1 - dim))
    return factor_of


def scatter_about(rng, dims, width, most, pieces=(), kind=jnp.bfloat16):
    entries = jax.random.normal(rng, dims, jnp.float32) * width
    if len(pieces) > 0:
        entries = levels(rng, dims, pieces, -0.22, 0.18) * entries
    return jnp.clip(entries, min=-most, max=most).astype(kind)


def setup_inputs(seed: int = 0, part: int = 0) -> dict:
    seeds = jax.random.split(jax.random.key(seed), 8)
    part_keys = jax.random.split(jax.random.fold_in(seeds[7], part), 8)
    return {
        "source_field": scatter_about(part_keys[0], (C, H, W), 1.0, 6.0, ((0, 2), (1, 4), (2, 2)), jnp.float32),
        "cotangent": scatter_about(part_keys[1], (C, H, W), 1.0, 6.0, ((0, 2), (1, 4), (2, 2)), jnp.float32),
        "spectral_weight": scatter_about(part_keys[2], (C, C, M, 2, KX), 2.0, 12.0, ((0, 2), (2, 2), (4, 4)), jnp.float32),
        "skip_gain": jnp.clip(jnp.exp(math.log(2.0) - 1.3862944 * jax.random.uniform(part_keys[3], (C,), jnp.float32) ** levels(part_keys[3], (C,), ((0, 2),), -0.2, 0.2)), 0.5, 2.0),
        "channel_bias": jnp.clip(jax.random.uniform(part_keys[4], (C,), jnp.float32, -0.5, 0.5) * levels(part_keys[4], (C,), ((0, 2),), -0.4, 0.0), -0.5, 0.5),
        "mode_limit": plant(jax.random.randint(part_keys[5], (C, 2), M // 2, M + 1), jax.random.fold_in(part_keys[5], 1), M // 2, M).astype(jnp.int32),
        "width_limit": plant(jax.random.randint(part_keys[6], (C,), C // 2, C + 1), jax.random.fold_in(part_keys[6], 1), C // 2, C).astype(jnp.int32),
    }


precise = lax.Precision.HIGHEST

def column_table(extent, freq_count, first_cell, cell_count):
    cell_index = first_cell + jnp.arange(cell_count, dtype=jnp.int32)
    wave_index = jnp.arange(freq_count, dtype=jnp.int32)
    products = (cell_index[:, None] * wave_index[None, :] % extent).astype(jnp.float32)
    angles = products * (2.0 * math.pi / extent)
    return jnp.stack([jnp.cos(angles), -jnp.sin(angles)], axis=-1).reshape(cell_count, 2 * freq_count)

def row_tables(extent, freq_count, first_cell, cell_count):
    cell_index = first_cell + jnp.arange(cell_count, dtype=jnp.int32)
    column = jnp.arange(2 * freq_count, dtype=jnp.int32)
    wave_index = (column + jnp.where(column >= freq_count, extent - 2 * freq_count, 0)).astype(jnp.int32)
    products = (cell_index[:, None] * wave_index[None, :] % extent).astype(jnp.float32)
    angles = products * (2.0 * math.pi / extent)
    return (jnp.cos(angles), jnp.sin(angles))

def spectrum(values, column_tab, row_cos, row_sin):
    channels, row_count, col_count = values.shape
    freq_count = column_tab.shape[1] // 2
    halves = jnp.einsum('chw,wk->chk', values, column_tab, precision=precise).reshape(channels, row_count, freq_count, 2)
    real_part = halves[..., 0]
    imag_part = halves[..., 1]
    out_real = jnp.einsum('chy,hx->cyx', real_part, row_cos, precision=precise) + jnp.einsum('chy,hx->cyx', imag_part, row_sin, precision=precise)
    out_imag = jnp.einsum('chy,hx->cyx', imag_part, row_cos, precision=precise) - jnp.einsum('chy,hx->cyx', real_part, row_sin, precision=precise)
    return jnp.stack([out_real, out_imag], axis=2)

def synthesis(modes_in, column_tab, row_cos, row_sin):
    channels = modes_in.shape[0]
    real_part = modes_in[:, :, 0]
    imag_part = modes_in[:, :, 1]
    back_real = jnp.einsum('cyx,hx->cyh', real_part, row_cos, precision=precise) - jnp.einsum('cyx,hx->cyh', imag_part, row_sin, precision=precise)
    back_imag = jnp.einsum('cyx,hx->cyh', real_part, row_sin, precision=precise) + jnp.einsum('cyx,hx->cyh', imag_part, row_cos, precision=precise)
    joined = jnp.stack([back_real, back_imag], axis=2).reshape(channels, -1, row_cos.shape[0])
    return jnp.einsum('ckh,wk->chw', joined, column_tab, precision=precise)

def contract(spectra, weight):
    spec_real = spectra[:, :, 0]
    spec_imag = spectra[:, :, 1]
    weight_real = weight[:, :, :, 0]
    weight_imag = weight[:, :, :, 1]
    out_real = jnp.einsum('iyx,ioyx->oyx', spec_real, weight_real, precision=precise) - jnp.einsum('iyx,ioyx->oyx', spec_imag, weight_imag, precision=precise)
    out_imag = jnp.einsum('iyx,ioyx->oyx', spec_real, weight_imag, precision=precise) + jnp.einsum('iyx,ioyx->oyx', spec_imag, weight_real, precision=precise)
    return jnp.stack([out_real, out_imag], axis=2)

def contract_back(grads, weight):
    grad_real = grads[:, :, 0]
    grad_imag = grads[:, :, 1]
    weight_real = weight[:, :, :, 0]
    weight_imag = weight[:, :, :, 1]
    back_real = jnp.einsum('oyx,ioyx->iyx', grad_real, weight_real, precision=precise) + jnp.einsum('oyx,ioyx->iyx', grad_imag, weight_imag, precision=precise)
    back_imag = jnp.einsum('oyx,ioyx->iyx', grad_imag, weight_real, precision=precise) - jnp.einsum('oyx,ioyx->iyx', grad_real, weight_imag, precision=precise)
    return jnp.stack([back_real, back_imag], axis=2)

def outer_grad(spectra, grads):
    spec_real = spectra[:, :, 0]
    spec_imag = spectra[:, :, 1]
    grad_real = grads[:, :, 0]
    grad_imag = grads[:, :, 1]
    real_side = jnp.einsum('iyx,oyx->ioyx', spec_real, grad_real) + jnp.einsum('iyx,oyx->ioyx', spec_imag, grad_imag)
    imag_side = jnp.einsum('iyx,oyx->ioyx', spec_real, grad_imag) - jnp.einsum('iyx,oyx->ioyx', spec_imag, grad_real)
    return jnp.stack([real_side, imag_side], axis=3)

def mode_weights(limit_rows, col_freq, row_freq, kx_count, cells_total):
    keep_cols = col_freq[None, :] < limit_rows[:, 0:1]
    keep_rows = (row_freq[None, :] < limit_rows[:, 1:2]) | ((kx_count - row_freq)[None, :] < limit_rows[:, 1:2])
    scales = jnp.where(col_freq == 0, 1.0, 2.0).astype(jnp.float32) / cells_total
    joined = keep_cols[:, :, None] & keep_rows[:, None, :]
    return (joined.astype(jnp.float32) * scales[None, :, None])[:, :, None, :]

def read_mask(in_index, width_limit):
    return (in_index[:, None] < width_limit[None, :]).astype(jnp.float32)[:, :, None, None, None]

def reference(source_field, cotangent, spectral_weight, skip_gain, channel_bias, mode_limit, width_limit):
    channels, row_count, col_count = source_field.shape
    freq_count = spectral_weight.shape[2]
    kx_count = spectral_weight.shape[4]
    column_tab = column_table(col_count, freq_count, 0, col_count)
    row_cos, row_sin = row_tables(row_count, freq_count, 0, row_count)
    weights = mode_weights(mode_limit, jnp.arange(freq_count, dtype=jnp.int32), jnp.arange(kx_count, dtype=jnp.int32), kx_count, row_count * col_count)
    reads = read_mask(jnp.arange(channels, dtype=jnp.int32), width_limit)
    masked_weight = spectral_weight * reads
    spectra = spectrum(source_field, column_tab, row_cos, row_sin)
    out_modes = contract(spectra, masked_weight) * weights
    branch = synthesis(out_modes, column_tab, row_cos, row_sin)
    skip_scale = skip_gain[:, None, None]
    summed = branch + skip_scale * source_field + channel_bias[:, None, None]
    output, gelu_back = jax.vjp(jax.nn.gelu, summed)
    grad_sum = gelu_back(cotangent)[0]
    grad_modes = spectrum(grad_sum, column_tab, row_cos, row_sin) * weights
    spectral_grad = outer_grad(spectra, grad_modes) * reads
    field_grad = synthesis(contract_back(grad_modes, masked_weight), column_tab, row_cos, row_sin) + skip_scale * grad_sum
    gate_grad = lax.optimization_barrier(jnp.sum(grad_sum * source_field, axis=(1, 2)))
    bias_grad = lax.optimization_barrier(jnp.sum(grad_sum, axis=(1, 2)))
    return (output, field_grad, spectral_grad, gate_grad, bias_grad)
```

```python
import functools
import math

import jax
import jax.numpy as jnp
from jax import lax
from jax.experimental import pallas as pl
from jax.experimental.pallas import tpu as pltpu
from jax.sharding import PartitionSpec as P

F32 = jnp.float32
BF16 = jnp.bfloat16
LANES = 128
GELU_A = math.sqrt(2.0 / math.pi)
GELU_B = GELU_A * 0.044715


def split(x):
    high = x.astype(BF16)
    return high, (x - high.astype(F32)).astype(BF16)


def split_table(x):
    high = lax.reduce_precision(x, 8, 7)
    return high.astype(BF16), (x - high).astype(BF16)


def mm(a, b):
    return jnp.dot(a, b, preferred_element_type=F32)


def angles(cells, freqs, extent):
    products = (cells[:, None] * freqs[None, :] % extent).astype(F32)
    return products * (2.0 * math.pi / extent)


def plan_tables(geo):
    col_cell = geo.mode * geo.cols + jnp.arange(geo.cols, dtype=jnp.int32)
    rel_mode = (geo.mode + jnp.arange(geo.modes, dtype=jnp.int32)) % geo.modes
    freq = (rel_mode[:, None] * geo.freq + jnp.arange(geo.freq, dtype=jnp.int32)[None, :])
    theta = angles(col_cell, freq.reshape(-1), geo.all_cols).reshape(geo.cols, geo.modes, geo.freq)
    cos, sin = jnp.cos(theta), jnp.sin(theta)
    first = jnp.stack([cos, -sin], axis=2).reshape(geo.cols, -1)
    second = jnp.stack([-sin, -cos], axis=2).reshape(geo.cols, -1)
    first_h, first_l = split_table(first)
    second_h, second_l = split_table(second)
    forward_cols = jnp.concatenate([first_h, first_l, second_h, second_l], axis=1)
    inverse_cols = jnp.stack(
        [
            jnp.concatenate([high.T, high.T, low.T, low.T], axis=0)
            for high, low in ((first_h, first_l), (second_h, second_l))
        ]
    )
    row_cell = geo.slab * geo.rows + jnp.arange(geo.rows, dtype=jnp.int32)
    rel_slab = (geo.slab + jnp.arange(geo.slabs, dtype=jnp.int32)) % geo.slabs
    place = (rel_slab[:, None] * geo.kx + jnp.arange(geo.kx, dtype=jnp.int32)[None, :]).reshape(-1)
    half = geo.slabs * geo.kx // 2
    wave = jnp.where(place < half, place, place - 2 * half)
    theta = angles(wave % geo.all_rows, row_cell, geo.all_rows)
    forward_h, forward_l = split_table(jnp.concatenate([jnp.cos(theta), jnp.sin(theta)], axis=1))
    forward_rows = jnp.concatenate([forward_h, forward_l], axis=0)
    kept = jnp.arange(geo.fold // 2, dtype=jnp.int32)
    theta = angles(row_cell, kept, geo.all_rows)
    live = (kept <= half)[None, :]
    inverse_h, inverse_l = split_table(
        jnp.concatenate(
            [jnp.where(live, jnp.cos(theta), 0.0), jnp.where(live, jnp.sin(theta), 0.0)], axis=1
        )
    )
    rest = jnp.zeros((geo.rows, 256 - 3 * geo.fold), BF16)
    inverse_rows = jnp.concatenate([inverse_h, inverse_h, inverse_l, rest], axis=1)
    same = (jnp.abs(wave)[None, :] == kept[:, None]).astype(F32)
    fold = jnp.concatenate([same, same * jnp.sign(wave).astype(F32)[None, :]], axis=0).astype(BF16)
    return forward_cols, forward_rows, inverse_cols, inverse_rows, jnp.concatenate([fold, fold], axis=1)


def lane_group(shape, width):
    return lax.broadcasted_iota(jnp.int32, shape, 1) // width


def emit_spectrum(parts, row_tab, own_ref, other_ref):
    kx_all = row_tab.shape[0] // 2
    doubled = []
    for first in range(0, len(parts), 2):
        pair = jnp.concatenate(
            [jnp.concatenate([a[:, :LANES], a[:, LANES:]], axis=0) for a in parts[first : first + 2]],
            axis=1,
        )
        high, low = split(pair)
        both = mm(row_tab, high)
        total = both[:kx_all] + both[kx_all:] + mm(row_tab[:kx_all], low)
        for lane in (0, LANES):
            one = total[:, lane : lane + LANES]
            doubled.append(one + pltpu.roll(one, 64, 1))
    turned = [pltpu.roll(s, 32, 1) for s in doubled]
    group = lane_group(doubled[0].shape, 32)

    def weave(arrays):
        return jnp.where(
            group == 0,
            arrays[0],
            jnp.where(group == 1, arrays[1], jnp.where(group == 2, arrays[2], arrays[3])),
        )

    own = weave([doubled[0], turned[1], doubled[2], turned[3]])
    other = weave([turned[0], doubled[1], turned[2], doubled[3]])
    slabs, _, kx, _ = own_ref.shape
    for q in range(slabs):
        own_ref[q, 0] = own[q * kx : (q + 1) * kx]
        other_ref[q, 0] = other[q * kx : (q + 1) * kx]


def forward_kernel(x_ref, col_ref, row_ref, own_ref, other_ref):
    parts = []
    for c in range(x_ref.shape[0]):
        high, low = split(x_ref[c])
        parts.append(mm(high, col_ref[...]) + mm(low, col_ref[...]))
    emit_spectrum(parts, row_ref[...], own_ref, other_ref)


def stack_modes(piece_refs, fold_ref, inv_col_ref, add=None):
    slabs = len(piece_refs) // 2
    halves = [
        jnp.concatenate([r[0] for r in piece_refs[m * slabs : (m + 1) * slabs]], axis=0) for m in (0, 1)
    ]
    high, low = split(jnp.concatenate(halves, axis=1))
    folded = mm(fold_ref[...], jnp.concatenate([high, low], axis=0))
    fold = folded.shape[0]
    group = lane_group((fold, LANES), 32)
    a, b = folded[:, :LANES], folded[:, LANES:]
    rows = []
    for c in range(4):
        a_at = [a if (t - c) % 4 == 0 else pltpu.roll(a, 32 * ((t - c) % 4), 1) for t in (0, 2)]
        b_at = [b if (t - c) % 4 == 0 else pltpu.roll(b, 32 * ((t - c) % 4), 1) for t in (1, 3)]
        one = jnp.where(
            group == 0, a_at[0], jnp.where(group == 1, b_at[0], jnp.where(group == 2, a_at[1], b_at[1]))
        )
        top = one.astype(BF16).astype(F32)
        rows.append(jnp.where(group < 2, top, one - top))
    half = fold // 2
    spread = []
    for side in (0, 1):
        lhs = jnp.concatenate([r[side * half : (side + 1) * half] for r in rows], axis=0).astype(BF16)
        spread.append(mm(jnp.concatenate([lhs, lhs], axis=1), inv_col_ref[side]))
    out = []
    for c in range(4):
        plus = spread[0][c * half : (c + 1) * half]
        if add is not None:
            plus = plus + jnp.where(lax.broadcasted_iota(jnp.int32, plus.shape, 0) == 0, add[c], 0.0)
        both = jnp.concatenate([plus, spread[1][c * half : (c + 1) * half]], axis=0)
        high, low = split(both)
        rest = jnp.zeros((256 - 3 * fold, both.shape[1]), BF16)
        out.append(jnp.concatenate([high, low, high, rest], axis=0))
    return out


CHUNK = 8


def middle_kernel(skip_ref, bias_ref, *refs, pieces):
    piece_refs = refs[:pieces]
    x_ref, ct_ref, fold_ref, inv_col_ref, inv_row_ref, col_ref, row_ref = refs[pieces : pieces + 7]
    out_ref, gs_ref, own_ref, other_ref, sums_ref, branch, high_ref, low_ref = refs[pieces + 7 :]
    step = pl.program_id(0)
    skips = [skip_ref[step * 4 + c] for c in range(4)]
    stacked = stack_modes(piece_refs, fold_ref, inv_col_ref, [bias_ref[step * 4 + c] for c in range(4)])
    rows, cols = x_ref.shape[1:]
    parts = []
    gate_rows, bias_rows = [], []
    for c in range(4):
        branch[c] = mm(inv_row_ref[...], stacked[c])
        gate = jnp.zeros((CHUNK, cols), F32)
        bias = jnp.zeros((CHUNK, cols), F32)
        for r in range(0, rows, CHUNK):
            x = x_ref[c, r : r + CHUNK]
            v = branch[c, r : r + CHUNK] + skips[c] * x
            q = v * v
            t = jnp.tanh(v * (q * GELU_B + GELU_A))
            s = 0.5 * t + 0.5
            out = v * s
            out_ref[c, r : r + CHUNK] = out
            slope = s + out * (1.0 - s) * (q * (6.0 * GELU_B) + 2.0 * GELU_A)
            grad = ct_ref[c, r : r + CHUNK] * slope
            gs_ref[c, r : r + CHUNK] = grad
            gate = gate + grad * x
            bias = bias + grad
            top = grad.astype(BF16)
            high_ref[c, r : r + CHUNK] = top
            low_ref[c, r : r + CHUNK] = (grad - top.astype(F32)).astype(BF16)
        parts.append(mm(high_ref[c], col_ref[...]) + mm(low_ref[c], col_ref[...]))
        for total, kept in ((gate, gate_rows), (bias, bias_rows)):
            line = jnp.sum(total, axis=0, keepdims=True)
            kept.append(sum(line[:, k : k + LANES] for k in range(0, cols, LANES)))
    emit_spectrum(parts, row_ref[...], own_ref, other_ref)
    sums_ref[0] = jnp.concatenate(gate_rows + bias_rows, axis=0)


def last_kernel(skip_ref, *refs, pieces):
    piece_refs = refs[:pieces]
    gs_ref, fold_ref, inv_col_ref, inv_row_ref, out_ref = refs[pieces:]
    step = pl.program_id(0)
    stacked = stack_modes(piece_refs, fold_ref, inv_col_ref)
    for c in range(4):
        out_ref[c] = mm(inv_row_ref[...], stacked[c]) + skip_ref[step * 4 + c] * gs_ref[c]


def limits_mask(place_ref, limit_ref, y, kx, kx_all, scale_cells, shape):
    col = place_ref[0] + y
    row = place_ref[1] + lax.broadcasted_iota(jnp.int32, shape, 0)
    wide = jnp.broadcast_to(limit_ref[0:1, :], shape)
    tall = jnp.broadcast_to(limit_ref[1:2, :], shape)
    keep = (col < wide) & ((row < tall) | (kx_all - row < tall))
    scale = jnp.where(col == 0, 1.0 / scale_cells, 2.0 / scale_cells).astype(F32)
    return jnp.where(keep, scale, 0.0)


def mix_kernel(place_ref, r0, r1, r2, r3, w_ref, limit_ref, width_ref, out_ref, spec_ref, acc, *, geo):
    freq = geo.freq
    block = w_ref.shape[1]
    step = pl.program_id(0)

    @pl.when(step == 0)
    def _():
        spec_ref[...] = r0[...] + r1[...] + r2[...] + r3[...]

    groups = spec_ref.shape[0]
    kx = geo.kx
    outs = w_ref.shape[4]
    for k in range(block):
        y = step * block + k
        shift = (LANES - y) % LANES
        re = jnp.zeros((kx, outs), F32)
        im = jnp.zeros((kx, outs), F32)
        for g in range(groups):
            line = pltpu.roll(spec_ref[g], shift, 1)
            for c in range(4):
                i = g * 4 + c
                sr = jnp.broadcast_to(line[:, 32 * c : 32 * c + 1], (kx, outs))
                si = jnp.broadcast_to(line[:, 32 * c + freq : 32 * c + freq + 1], (kx, outs))
                reads = jnp.broadcast_to(place_ref[2] + i < width_ref[0:1, :], (kx, outs))
                wr = jnp.where(reads, w_ref[i, k, 0], 0.0)
                wi = jnp.where(reads, w_ref[i, k, 1], 0.0)
                re = re + (sr * wr - si * wi)
                im = im + (sr * wi + si * wr)
        mask = limits_mask(place_ref, limit_ref, y, kx, geo.kx_all, geo.cells, (kx, outs))
        out_ref[k, 0] = re * mask
        out_ref[k, 1] = im * mask


def back_kernel(place_ref, g_ref, w_ref, limit_ref, width_ref, out_ref, gm_ref, *, geo):
    freq = geo.freq
    block = w_ref.shape[1]
    step = pl.program_id(0)
    kx = geo.kx
    outs = w_ref.shape[4]
    groups = out_ref.shape[0]
    lane = lax.broadcasted_iota(jnp.int32, (kx, LANES), 1)

    @pl.when(step == 0)
    def _():
        out_ref[...] = jnp.zeros_like(out_ref)

    for k in range(block):
        y = step * block + k
        mask = limits_mask(place_ref, limit_ref, y, kx, geo.kx_all, geo.cells, (kx, outs))
        gr = g_ref[k, 0] * mask
        gi = g_ref[k, 1] * mask
        gm_ref[k, 0] = gr
        gm_ref[k, 1] = gi
        for g in range(groups):
            line = out_ref[g]
            for c in range(4):
                i = g * 4 + c
                reads = jnp.broadcast_to(place_ref[2] + i < width_ref[0:1, :], (kx, outs))
                wr = jnp.where(reads, w_ref[i, k, 0], 0.0)
                wi = jnp.where(reads, w_ref[i, k, 1], 0.0)
                br = jnp.sum(gr * wr + gi * wi, axis=1, keepdims=True)
                bi = jnp.sum(gi * wr - gr * wi, axis=1, keepdims=True)
                line = jnp.where(lane == 32 * c + y, jnp.broadcast_to(br, (kx, LANES)), line)
                line = jnp.where(lane == 32 * c + freq + y, jnp.broadcast_to(bi, (kx, LANES)), line)
            out_ref[g] = line


def outer_kernel(place_ref, spec_ref, gm_ref, width_ref, out_ref, *, geo):
    freq = geo.freq
    block = out_ref.shape[1]
    step = pl.program_id(0)
    kx = geo.kx
    outs = out_ref.shape[4]
    for k in range(block):
        y = step * block + k
        shift = (LANES - y) % LANES
        gr = gm_ref[k, 0]
        gi = gm_ref[k, 1]
        for g in range(spec_ref.shape[0]):
            line = pltpu.roll(spec_ref[g], shift, 1)
            for c in range(4):
                i = g * 4 + c
                sr = jnp.broadcast_to(line[:, 32 * c : 32 * c + 1], (kx, outs))
                si = jnp.broadcast_to(line[:, 32 * c + freq : 32 * c + freq + 1], (kx, outs))
                reads = jnp.broadcast_to(place_ref[2] + i < width_ref[0:1, :], (kx, outs))
                out_ref[i, k, 0] = jnp.where(reads, sr * gr + si * gi, 0.0)
                out_ref[i, k, 1] = jnp.where(reads, sr * gi - si * gr, 0.0)


class Geometry:
    def __init__(self, field, weight):
        self.channels, self.rows, self.cols = field.shape
        self.outs, self.freq, self.kx = weight.shape[1], weight.shape[2], weight.shape[4]
        self.slabs = lax.axis_size("slab")
        self.modes = lax.axis_size("mode")
        self.chans = lax.axis_size("chan")
        self.slab = lax.axis_index("slab")
        self.mode = lax.axis_index("mode")
        self.chan = lax.axis_index("chan")
        self.kx_all = self.kx * self.slabs
        self.all_rows = self.rows * self.slabs
        self.all_cols = self.cols * self.modes
        self.cells = float(self.all_rows * self.all_cols)
        self.fold = 16 * ((2 * (self.kx_all // 2 + 1) + 15) // 16)

    def fits(self):
        return (
            self.modes == 2
            and self.chans == 2
            and self.slabs == 4
            and self.freq == 16
            and self.kx_all == 64
            and self.kx % 8 == 0
            and self.channels % 4 == 0
            and self.rows % 16 == 0
            and self.cols % LANES == 0
            and 3 * self.fold <= 256
        )


def swap(x, name):
    n = lax.axis_size(name)
    return lax.ppermute(x, name, [(i, (i + 1) % n) for i in range(n)])


def fetch(x, name, distance):
    n = lax.axis_size(name)
    return lax.ppermute(x, name, [((i + distance) % n, i) for i in range(n)])


def send(x, name, distance):
    n = lax.axis_size(name)
    return lax.ppermute(x, name, [(i, (i + distance) % n) for i in range(n)])


def whole(shape):
    return pl.BlockSpec(shape, lambda *_: (0,) * len(shape))


SMEM = pl.BlockSpec(memory_space=pltpu.SMEM)


def params(limit):
    return pltpu.CompilerParams(dimension_semantics=("arbitrary",), vmem_limit_bytes=limit)


def spectrum_shapes(geo):
    groups = geo.channels // 4
    shape = (geo.slabs, groups, geo.kx, LANES)
    block = (geo.slabs, 1, geo.kx, LANES)
    return [jax.ShapeDtypeStruct(shape, F32)] * 2, [pl.BlockSpec(block, lambda s: (0, s, 0, 0))] * 2


def reduce_spectrum(own, other, geo):
    own = own + swap(other, "mode")
    return [own[0]] + [send(own[d], "slab", d) for d in range(1, geo.slabs)]


def gather_modes(mine, geo):
    near = [mine] + [fetch(mine, "slab", d) for d in range(1, geo.slabs)]
    return near + [swap(piece, "mode") for piece in near]


def fast_local(
    source_field, cotangent, spectral_weight, skip_gain, channel_bias, mode_limit, width_limit, geo
):
    channels, rows, cols = source_field.shape
    groups = channels // 4
    fwd_cols, fwd_rows, inv_cols, inv_rows, fold = plan_tables(geo)
    weight = jnp.transpose(spectral_weight, (0, 2, 3, 4, 1))
    field_spec = pl.BlockSpec((4, rows, cols), lambda s: (s, 0, 0))
    piece_spec = pl.BlockSpec((1, geo.kx, LANES), lambda s: (s, 0, 0))
    spec_shapes, spec_specs = spectrum_shapes(geo)
    place = jnp.stack([geo.mode * geo.freq, geo.slab * geo.kx, geo.chan * channels]).astype(jnp.int32)
    limits = jnp.transpose(mode_limit)
    widths = width_limit[None, :]

    own, other = pl.pallas_call(
        forward_kernel,
        grid=(groups,),
        in_specs=[field_spec, whole(fwd_cols.shape), whole(fwd_rows.shape)],
        out_specs=spec_specs,
        out_shape=spec_shapes,
        compiler_params=params(40 << 20),
        name="forward",
    )(source_field, fwd_cols, fwd_rows)
    parts = reduce_spectrum(own, other, geo)

    block = 4
    steps = geo.freq // block
    w_spec = pl.BlockSpec((channels, block, 2, geo.kx, geo.outs), lambda s: (0, s, 0, 0, 0))
    g_spec = pl.BlockSpec((block, 2, geo.kx, geo.outs), lambda s: (s, 0, 0, 0))
    piece = (groups, geo.kx, LANES)
    piece_shape = jax.ShapeDtypeStruct(piece, F32)
    modes_shape = jax.ShapeDtypeStruct((geo.freq, 2, geo.kx, geo.outs), F32)
    mixed, spectra = pl.pallas_call(
        functools.partial(mix_kernel, geo=geo),
        grid=(steps,),
        in_specs=[SMEM] + [whole(piece)] * 4 + [w_spec, whole(limits.shape), whole(widths.shape)],
        out_specs=[g_spec, whole(piece)],
        out_shape=[modes_shape, piece_shape],
        scratch_shapes=[pltpu.VMEM((8, LANES), F32)],
        compiler_params=params(40 << 20),
        name="mix",
    )(place, *parts, weight, limits, widths)
    laid = mixed.reshape(geo.freq, 2, geo.kx, geo.chans, groups, 4)
    laid = laid.transpose(3, 4, 2, 5, 1, 0).reshape((geo.chans,) + piece)
    mine = lax.dynamic_index_in_dim(laid, geo.chan, 0, keepdims=False)
    theirs = lax.dynamic_index_in_dim(laid, 1 - geo.chan, 0, keepdims=False)
    pieces = gather_modes(mine + swap(theirs, "chan"), geo)

    out_field = jax.ShapeDtypeStruct(source_field.shape, F32)
    output, grad_sum, own, other, sums = pl.pallas_call(
        functools.partial(middle_kernel, pieces=len(pieces)),
        grid=(groups,),
        in_specs=[SMEM, SMEM]
        + [piece_spec] * len(pieces)
        + [field_spec, field_spec]
        + [whole(t.shape) for t in (fold, inv_cols, inv_rows, fwd_cols, fwd_rows)],
        out_specs=[field_spec, field_spec] + spec_specs + [pl.BlockSpec((1, 8, LANES), lambda s: (s, 0, 0))],
        out_shape=[out_field, out_field] + spec_shapes + [jax.ShapeDtypeStruct((groups, 8, LANES), F32)],
        scratch_shapes=[
            pltpu.VMEM((4, rows, cols), F32),
            pltpu.VMEM((4, rows, cols), BF16),
            pltpu.VMEM((4, rows, cols), BF16),
        ],
        compiler_params=params(56 << 20),
        name="middle",
    )(
        skip_gain, channel_bias, *pieces, source_field, cotangent, fold, inv_cols, inv_rows, fwd_cols, fwd_rows
    )
    parts = reduce_spectrum(own, other, geo)
    grads = parts[0] + parts[1] + parts[2] + parts[3]
    peer = swap(grads, "chan")
    first = geo.chan == 0
    laid = jnp.stack([jnp.where(first, grads, peer), jnp.where(first, peer, grads)])
    laid = laid.reshape(geo.chans, groups, geo.kx, 4, 2, geo.freq).transpose(5, 4, 2, 0, 1, 3)
    laid = laid.reshape(geo.freq, 2, geo.kx, geo.outs)
    back, grad_modes = pl.pallas_call(
        functools.partial(back_kernel, geo=geo),
        grid=(steps,),
        in_specs=[SMEM, g_spec, w_spec, whole(limits.shape), whole(widths.shape)],
        out_specs=[whole(piece), g_spec],
        out_shape=[piece_shape, modes_shape],
        compiler_params=params(40 << 20),
        name="back",
    )(place, laid, weight, limits, widths)
    pieces = gather_modes(back, geo)
    spectral_grad = pl.pallas_call(
        functools.partial(outer_kernel, geo=geo),
        grid=(steps,),
        in_specs=[SMEM, whole(piece), g_spec, whole(widths.shape)],
        out_specs=w_spec,
        out_shape=jax.ShapeDtypeStruct(weight.shape, F32),
        compiler_params=params(40 << 20),
        cost_estimate=pl.CostEstimate(flops=200_000_000, bytes_accessed=8 << 20, transcendentals=0),
        name="outer",
    )(place, spectra, grad_modes, widths)
    field_grad = pl.pallas_call(
        functools.partial(last_kernel, pieces=len(pieces)),
        grid=(groups,),
        in_specs=[SMEM]
        + [piece_spec] * len(pieces)
        + [field_spec]
        + [whole(t.shape) for t in (fold, inv_cols, inv_rows)],
        out_specs=field_spec,
        out_shape=out_field,
        compiler_params=params(48 << 20),
        name="last",
    )(skip_gain, *pieces, grad_sum, fold, inv_cols, inv_rows)
    sums = jnp.sum(sums, axis=2)
    sums = sums + swap(sums, "mode")
    sums = sums + send(sums, "slab", 1) + send(sums, "slab", 2) + send(sums, "slab", 3)
    gate_grad = sums[:, :4].reshape(channels)
    bias_grad = sums[:, 4:].reshape(channels)
    return (output, field_grad, jnp.transpose(spectral_grad, (0, 4, 1, 2, 3)), gate_grad, bias_grad)


precise = lax.Precision.HIGHEST


def column_table(extent, freq_count, first_cell, cell_count):
    cell_index = first_cell + jnp.arange(cell_count, dtype=jnp.int32)
    wave_index = jnp.arange(freq_count, dtype=jnp.int32)
    products = (cell_index[:, None] * wave_index[None, :] % extent).astype(jnp.float32)
    angles = products * (2.0 * math.pi / extent)
    return jnp.stack([jnp.cos(angles), -jnp.sin(angles)], axis=-1).reshape(
        cell_count, 2 * freq_count
    )


def row_tables(extent, freq_count, first_cell, cell_count):
    cell_index = first_cell + jnp.arange(cell_count, dtype=jnp.int32)
    column = jnp.arange(2 * freq_count, dtype=jnp.int32)
    wave_index = column + jnp.where(column >= freq_count, extent - 2 * freq_count, 0)
    products = (cell_index[:, None] * wave_index[None, :] % extent).astype(jnp.float32)
    angles = products * (2.0 * math.pi / extent)
    return (jnp.cos(angles), jnp.sin(angles))


def row_forward(lined, row_cos, row_sin):
    line_real = lined[:, 0]
    line_imag = lined[:, 1]
    out_real = jnp.dot(line_real, row_cos, precision=precise) + jnp.dot(
        line_imag, row_sin, precision=precise
    )
    out_imag = jnp.dot(line_imag, row_cos, precision=precise) - jnp.dot(
        line_real, row_sin, precision=precise
    )
    return jnp.stack([out_real, out_imag], axis=1)


def row_inverse(modes_in, row_cos, row_sin):
    mode_real = modes_in[:, 0]
    mode_imag = modes_in[:, 1]
    back_real = jnp.dot(mode_real, row_cos.T, precision=precise) - jnp.dot(
        mode_imag, row_sin.T, precision=precise
    )
    back_imag = jnp.dot(mode_real, row_sin.T, precision=precise) + jnp.dot(
        mode_imag, row_cos.T, precision=precise
    )
    return jnp.stack([back_real, back_imag], axis=1)


def contract(spectra, weight):
    spec_real = spectra[:, :, 0]
    spec_imag = spectra[:, :, 1]
    weight_real = weight[:, :, :, 0]
    weight_imag = weight[:, :, :, 1]
    out_real = jnp.einsum("iyx,ioyx->oyx", spec_real, weight_real, precision=precise) - jnp.einsum(
        "iyx,ioyx->oyx", spec_imag, weight_imag, precision=precise
    )
    out_imag = jnp.einsum("iyx,ioyx->oyx", spec_real, weight_imag, precision=precise) + jnp.einsum(
        "iyx,ioyx->oyx", spec_imag, weight_real, precision=precise
    )
    return jnp.stack([out_real, out_imag], axis=2)


def contract_back(grads, weight):
    grad_real = grads[:, :, 0]
    grad_imag = grads[:, :, 1]
    weight_real = weight[:, :, :, 0]
    weight_imag = weight[:, :, :, 1]
    back_real = jnp.einsum("oyx,ioyx->iyx", grad_real, weight_real, precision=precise) + jnp.einsum(
        "oyx,ioyx->iyx", grad_imag, weight_imag, precision=precise
    )
    back_imag = jnp.einsum("oyx,ioyx->iyx", grad_imag, weight_real, precision=precise) - jnp.einsum(
        "oyx,ioyx->iyx", grad_real, weight_imag, precision=precise
    )
    return jnp.stack([back_real, back_imag], axis=2)


def outer_grad(spectra, grads):
    spec_real = spectra[:, :, 0]
    spec_imag = spectra[:, :, 1]
    grad_real = grads[:, :, 0]
    grad_imag = grads[:, :, 1]
    real_side = jnp.einsum("iyx,oyx->ioyx", spec_real, grad_real) + jnp.einsum(
        "iyx,oyx->ioyx", spec_imag, grad_imag
    )
    imag_side = jnp.einsum("iyx,oyx->ioyx", spec_real, grad_imag) - jnp.einsum(
        "iyx,oyx->ioyx", spec_imag, grad_real
    )
    return jnp.stack([real_side, imag_side], axis=3)


def mode_weights(limit_rows, col_freq, row_freq, kx_count, cells_total):
    keep_cols = col_freq[None, :] < limit_rows[:, 0:1]
    keep_rows = (row_freq[None, :] < limit_rows[:, 1:2]) | (
        (kx_count - row_freq)[None, :] < limit_rows[:, 1:2]
    )
    scales = jnp.where(col_freq == 0, 1.0, 2.0).astype(jnp.float32) / cells_total
    joined = keep_cols[:, :, None] & keep_rows[:, None, :]
    return (joined.astype(jnp.float32) * scales[None, :, None])[:, :, None, :]


def read_mask(in_index, width_limit):
    return (in_index[:, None] < width_limit[None, :]).astype(jnp.float32)[:, :, None, None, None]


def plain_local(
    source_field, cotangent, spectral_weight, skip_gain, channel_bias, mode_limit, width_limit
):
    channels, row_count, col_count = source_field.shape
    slab_count = lax.axis_size("slab")
    mode_count = lax.axis_size("mode")
    slab_index = lax.axis_index("slab")
    mode_index = lax.axis_index("mode")
    chan_index = lax.axis_index("chan")
    local_freq = spectral_weight.shape[2]
    local_kx = spectral_weight.shape[4]
    freq_count = local_freq * mode_count
    kx_count = local_kx * slab_count
    all_rows = row_count * slab_count
    all_cols = col_count * mode_count
    column_tab = column_table(all_cols, freq_count, mode_index * col_count, col_count)
    row_cos, row_sin = row_tables(all_rows, freq_count, slab_index * row_count, row_count)

    def spectrum(values):
        partial_cols = jnp.einsum("chw,wk->ckh", values, column_tab, precision=precise)
        summed_cols = lax.psum_scatter(partial_cols, "mode", scatter_dimension=1, tiled=True)
        paired = summed_cols.reshape(values.shape[0] * local_freq, 2, row_count)
        spectra = lax.psum_scatter(
            row_forward(paired, row_cos, row_sin), "slab", scatter_dimension=2, tiled=True
        )
        return spectra.reshape(values.shape[0], local_freq, 2, local_kx)

    def synthesis(modes_in):
        whole_modes = lax.all_gather(modes_in, "slab", axis=3, tiled=True)
        rebuilt = row_inverse(
            whole_modes.reshape(channels * local_freq, 2, kx_count), row_cos, row_sin
        )
        rebuilt = rebuilt.reshape(channels, 2 * local_freq, row_count)
        gathered = lax.all_gather(rebuilt, "mode", axis=1, tiled=True)
        return jnp.einsum("ckh,wk->chw", gathered, column_tab, precision=precise)

    in_index = chan_index * channels + jnp.arange(channels, dtype=jnp.int32)
    col_freq = mode_index * local_freq + jnp.arange(local_freq, dtype=jnp.int32)
    row_freq = slab_index * local_kx + jnp.arange(local_kx, dtype=jnp.int32)
    limit_rows = lax.dynamic_slice_in_dim(mode_limit, chan_index * channels, channels, 0)
    weights = mode_weights(limit_rows, col_freq, row_freq, kx_count, all_rows * all_cols)
    reads = read_mask(in_index, width_limit)
    masked_weight = spectral_weight * reads
    spectra = spectrum(source_field)
    out_modes = (
        lax.psum_scatter(contract(spectra, masked_weight), "chan", scatter_dimension=0, tiled=True)
        * weights
    )
    branch = synthesis(out_modes)
    skip_scale = skip_gain[:, None, None]
    summed = branch + skip_scale * source_field + channel_bias[:, None, None]
    output, gelu_back = jax.vjp(jax.nn.gelu, summed)
    grad_sum = gelu_back(cotangent)[0]
    grad_modes = spectrum(grad_sum) * weights
    all_grads = lax.all_gather(grad_modes, "chan", axis=0, tiled=True)
    spectral_grad = outer_grad(spectra, all_grads) * reads
    field_grad = synthesis(contract_back(all_grads, masked_weight)) + skip_scale * grad_sum
    gate_grad, bias_grad = lax.psum(
        (jnp.sum(grad_sum * source_field, axis=(1, 2)), jnp.sum(grad_sum, axis=(1, 2))),
        ("slab", "mode"),
    )
    return (output, field_grad, spectral_grad, gate_grad, bias_grad)


def local(*args):
    geo = Geometry(args[0], args[2])
    if geo.fits():
        return fast_local(*args, geo)
    return plain_local(*args)


def solution(mesh):
    in_specs = (
        P(("member", "chan"), "slab", "mode"),
        P(("member", "chan"), "slab", "mode"),
        P(("member", "chan"), None, "mode", None, "slab"),
        P(("member", "chan")),
        P(("member", "chan")),
        P("member", None),
        P("member"),
    )
    out_specs = (
        P(("member", "chan"), "slab", "mode"),
        P(("member", "chan"), "slab", "mode"),
        P(("member", "chan"), None, "mode", None, "slab"),
        P(("member", "chan")),
        P(("member", "chan")),
    )
    return jax.shard_map(local, mesh=mesh, in_specs=in_specs, out_specs=out_specs, check_vma=False)
```

```python
import functools
import math

import jax
import jax.numpy as jnp
from jax import lax
from jax.experimental import pallas as pl
from jax.experimental.pallas import tpu as pltpu
from jax.sharding import PartitionSpec as P

F32 = jnp.float32
BF16 = jnp.bfloat16
LANES = 128
GELU_A = math.sqrt(2.0 / math.pi)
GELU_B = GELU_A * 0.044715


def split(x):
    high = x.astype(BF16)
    return high, (x - high.astype(F32)).astype(BF16)


def split_table(x):
    high = lax.reduce_precision(x, 8, 7)
    return high.astype(BF16), (x - high).astype(BF16)


def mm(a, b):
    return jnp.dot(a, b, preferred_element_type=F32)


def angles(cells, freqs, extent):
    products = (cells[:, None] * freqs[None, :] % extent).astype(F32)
    return products * (2.0 * math.pi / extent)


def plan_tables(geo):
    col_cell = geo.mode * geo.cols + jnp.arange(geo.cols, dtype=jnp.int32)
    rel_mode = (geo.mode + jnp.arange(geo.modes, dtype=jnp.int32)) % geo.modes
    freq = (rel_mode[:, None] * geo.freq + jnp.arange(geo.freq, dtype=jnp.int32)[None, :])
    theta = angles(col_cell, freq.reshape(-1), geo.all_cols).reshape(geo.cols, geo.modes, geo.freq)
    cos, sin = jnp.cos(theta), jnp.sin(theta)
    first = jnp.stack([cos, -sin], axis=2).reshape(geo.cols, -1)
    second = jnp.stack([-sin, -cos], axis=2).reshape(geo.cols, -1)
    first_h, first_l = split_table(first)
    second_h, second_l = split_table(second)
    forward_cols = jnp.concatenate([first_h, first_l, second_h, second_l], axis=1)
    inverse_cols = jnp.stack(
        [
            jnp.concatenate([high.T, high.T, low.T, low.T], axis=0)
            for high, low in ((first_h, first_l), (second_h, second_l))
        ]
    )
    row_cell = geo.slab * geo.rows + jnp.arange(geo.rows, dtype=jnp.int32)
    rel_slab = (geo.slab + jnp.arange(geo.slabs, dtype=jnp.int32)) % geo.slabs
    place = (rel_slab[:, None] * geo.kx + jnp.arange(geo.kx, dtype=jnp.int32)[None, :]).reshape(-1)
    half = geo.slabs * geo.kx // 2
    wave = jnp.where(place < half, place, place - 2 * half)
    theta = angles(wave % geo.all_rows, row_cell, geo.all_rows)
    forward_h, forward_l = split_table(jnp.concatenate([jnp.cos(theta), jnp.sin(theta)], axis=1))
    forward_rows = jnp.concatenate([forward_h, forward_l], axis=0)
    kept = jnp.arange(geo.fold // 2, dtype=jnp.int32)
    theta = angles(row_cell, kept, geo.all_rows)
    live = (kept <= half)[None, :]
    inverse_h, inverse_l = split_table(
        jnp.concatenate(
            [jnp.where(live, jnp.cos(theta), 0.0), jnp.where(live, jnp.sin(theta), 0.0)], axis=1
        )
    )
    rest = jnp.zeros((geo.rows, 256 - 3 * geo.fold), BF16)
    inverse_rows = jnp.concatenate([inverse_h, inverse_h, inverse_l, rest], axis=1)
    same = (jnp.abs(wave)[None, :] == kept[:, None]).astype(F32)
    fold = jnp.concatenate([same, same * jnp.sign(wave).astype(F32)[None, :]], axis=0).astype(BF16)
    return forward_cols, forward_rows, inverse_cols, inverse_rows, jnp.concatenate([fold, fold], axis=1)


def lane_group(shape, width):
    return lax.broadcasted_iota(jnp.int32, shape, 1) // width


def pair_spectra(first, second, row_tab):
    kx_all = row_tab.shape[0] // 2
    pair = jnp.concatenate(
        [jnp.concatenate([a[:, :LANES], a[:, LANES:]], axis=0) for a in (first, second)], axis=1
    )
    high, low = split(pair)
    both = mm(row_tab, high)
    total = both[:kx_all] + both[kx_all:] + mm(row_tab[:kx_all], low)
    halves = [total[:, lane : lane + LANES] for lane in (0, LANES)]
    return [one + pltpu.roll(one, 64, 1) for one in halves]


def write_spectra(doubled, own_ref, other_ref, group):
    turned = [pltpu.roll(s, 32, 1) for s in doubled]
    place = lane_group(doubled[0].shape, 32)

    def weave(arrays):
        return jnp.where(
            place == 0,
            arrays[0],
            jnp.where(place == 1, arrays[1], jnp.where(place == 2, arrays[2], arrays[3])),
        )

    own = weave([doubled[0], turned[1], doubled[2], turned[3]])
    other = weave([turned[0], doubled[1], turned[2], doubled[3]])
    slabs, _, kx, _ = own_ref.shape
    for q in range(slabs):
        own_ref[q, group] = own[q * kx : (q + 1) * kx]
        other_ref[q, group] = other[q * kx : (q + 1) * kx]


def forward_kernel(place_ref, x_ref, col_ref, row_ref, own_ref, other_ref, keep_ref, sems):
    del place_ref
    step = pl.program_id(0)

    def fetching(at):
        four = pl.ds(at * 4, 4)
        return pltpu.make_async_copy(x_ref.at[four], keep_ref.at[four], sems.at[at])

    @pl.when(step == 0)
    def _():
        for at in range(sems.shape[0]):
            fetching(at).start()

    fetching(step).wait()
    parts = []
    for c in range(4):
        high, low = split(keep_ref[step * 4 + c])
        parts.append(mm(high, col_ref[...]) + mm(low, col_ref[...]))
    doubled = pair_spectra(*parts[:2], row_ref[...]) + pair_spectra(*parts[2:], row_ref[...])
    write_spectra(doubled, own_ref, other_ref, step)


def fold_modes(piece_refs, step, fold_ref):
    slabs = len(piece_refs) // 2
    halves = [
        jnp.concatenate([r[step] for r in piece_refs[m * slabs : (m + 1) * slabs]], axis=0) for m in (0, 1)
    ]
    high, low = split(jnp.concatenate(halves, axis=1))
    return mm(fold_ref[...], jnp.concatenate([high, low], axis=0))


def line_up(folded, c):
    group = lane_group((folded.shape[0], LANES), 32)
    a, b = folded[:, :LANES], folded[:, LANES:]
    a_at = [a if (t - c) % 4 == 0 else pltpu.roll(a, 32 * ((t - c) % 4), 1) for t in (0, 2)]
    b_at = [b if (t - c) % 4 == 0 else pltpu.roll(b, 32 * ((t - c) % 4), 1) for t in (1, 3)]
    one = jnp.where(
        group == 0, a_at[0], jnp.where(group == 1, b_at[0], jnp.where(group == 2, a_at[1], b_at[1]))
    )
    top = one.astype(BF16).astype(F32)
    return jnp.where(group < 2, top, one - top)


def spread_columns(rows, side, inv_col_ref):
    half = rows[0].shape[0] // 2
    lhs = jnp.concatenate([r[side * half : (side + 1) * half] for r in rows], axis=0).astype(BF16)
    return mm(jnp.concatenate([lhs, lhs], axis=1), inv_col_ref[side])


def stack_operand(plus, minus, add=None):
    if add is not None:
        plus = plus + jnp.where(lax.broadcasted_iota(jnp.int32, plus.shape, 0) == 0, add, 0.0)
    high, low = split(jnp.concatenate([plus, minus], axis=0))
    rest = jnp.zeros((256 - 3 * high.shape[0], high.shape[1]), BF16)
    return jnp.concatenate([high, low, high, rest], axis=0)


def stack_modes(piece_refs, step, fold_ref, inv_col_ref):
    folded = fold_modes(piece_refs, step, fold_ref)
    half = folded.shape[0] // 2
    rows = [line_up(folded, c) for c in range(4)]
    sides = [spread_columns(rows, side, inv_col_ref) for side in (0, 1)]
    return [stack_operand(*(s[c * half : (c + 1) * half] for s in sides)) for c in range(4)]


CHUNK = 16


def middle_kernel(skip_ref, bias_ref, *refs, pieces):
    piece_refs = refs[:pieces]
    x_ref, ct_ref, fold_ref, inv_col_ref, inv_row_ref, col_ref, row_ref = refs[pieces : pieces + 7]
    out_ref, gs_ref, own_ref, other_ref, ready, wide_ref, branch, high_ref, low_ref, part_ref = refs[pieces + 7 :]
    step = pl.program_id(0)
    last = pl.num_programs(0) - 1
    rows, cols = x_ref.shape[1:]
    sums = own_ref.shape[1] - 1
    half = fold_ref.shape[0] // 2

    def preparing(at):
        held = {}

        def begin():
            held["folded"] = fold_modes(piece_refs, at, fold_ref)

        def line(c):
            held[c] = line_up(held["folded"], c)

        def spread(side):
            wide_ref[side] = spread_columns([held[c] for c in range(4)], side, inv_col_ref)

        def stack(c):
            plus, minus = (wide_ref[side, c * half : (c + 1) * half] for side in (0, 1))
            ready[c] = stack_operand(plus, minus, bias_ref[at * 4 + c])

        early = [begin] + [functools.partial(line, c) for c in range(4)]
        early += [functools.partial(spread, side) for side in (0, 1)]
        return early, [functools.partial(stack, c) for c in range(4)]

    def emitting(at):
        held = {}

        def pair(k):
            held[k] = pair_spectra(part_ref[2 * k], part_ref[2 * k + 1], row_ref[...])

        def write():
            write_spectra(held[0] + held[1], own_ref, other_ref, at)

        return [functools.partial(pair, 0), functools.partial(pair, 1), write]

    @pl.when(step == 0)
    def _():
        early, late = preparing(0)
        for task in early + late:
            task()
        part_ref[...] = jnp.zeros_like(part_ref)
        own_ref[0, sums] = jnp.zeros(own_ref.shape[2:], F32)

    early, late = preparing(jnp.minimum(step + 1, last))
    emits = emitting(jnp.maximum(step - 1, 0))
    chunks = rows // CHUNK
    plan = {(0, 1): emits[0], (0, 5): emits[1], (0, 10): emits[2]}
    for k, task in enumerate(early):
        plan[(1 + k // 4, 2 + 3 * (k % 4))] = task
    for k, task in enumerate(late):
        plan[(3, 2 + 3 * k)] = task
    tile = own_ref[0, sums]
    row = lax.broadcasted_iota(jnp.int32, tile.shape, 0)
    lane = lax.broadcasted_iota(jnp.int32, tile.shape, 1)
    branch[0] = mm(inv_row_ref[...], ready[0])
    for c in range(4):
        channel = step * 4 + c
        skip = skip_ref[channel]
        gate = jnp.zeros((CHUNK, cols), F32)
        bias = jnp.zeros((CHUNK, cols), F32)
        for k in range(chunks):
            r = k * CHUNK
            if (c, k) in plan:
                plan[(c, k)]()
            if k == 0 and c < 3:
                branch[c + 1] = mm(inv_row_ref[...], ready[c + 1])
            if k == 1 and c > 0:
                part_ref[c - 1] = mm(high_ref[c - 1], col_ref[...]) + mm(low_ref[c - 1], col_ref[...])
            x = x_ref[channel, r : r + CHUNK]
            v = branch[c, r : r + CHUNK] + skip * x
            q = v * v
            t = jnp.tanh(v * (q * GELU_B + GELU_A))
            s = 0.5 * t + 0.5
            out = v * s
            out_ref[c, r : r + CHUNK] = out
            slope = s + out * (1.0 - s) * (q * (6.0 * GELU_B) + 2.0 * GELU_A)
            grad = ct_ref[c, r : r + CHUNK] * slope
            gs_ref[channel, r : r + CHUNK] = grad
            gate = gate + grad * x
            bias = bias + grad
            top = grad.astype(BF16)
            high_ref[c, r : r + CHUNK] = top
            low_ref[c, r : r + CHUNK] = (grad - top.astype(F32)).astype(BF16)
        for at, total in ((0, gate), (1, bias)):
            line = jnp.sum(total, axis=0, keepdims=True)
            value = jnp.sum(sum(line[:, k : k + LANES] for k in range(0, cols, LANES)), axis=1, keepdims=True)
            tile = jnp.where((row == at) & (lane == channel), jnp.broadcast_to(value, tile.shape), tile)
    part_ref[3] = mm(high_ref[3], col_ref[...]) + mm(low_ref[3], col_ref[...])
    own_ref[0, sums] = tile

    @pl.when(step == last)
    def _():
        for task in emitting(last):
            task()
        for q in range(own_ref.shape[0]):
            own_ref[q, sums] = tile
            other_ref[q, sums] = tile


def last_kernel(skip_ref, *refs, pieces):
    piece_refs = refs[:pieces]
    gs_ref, fold_ref, inv_col_ref, inv_row_ref, out_ref = refs[pieces:]
    step = pl.program_id(0)
    block = out_ref.shape[0]
    for first in range(0, block, 4):
        stacked = stack_modes(piece_refs, step * (block // 4) + first // 4, fold_ref, inv_col_ref)
        for c in range(4):
            channel = step * block + first + c
            out_ref[first + c] = mm(inv_row_ref[...], stacked[c]) + skip_ref[channel] * gs_ref[channel]


def limits_mask(place_ref, limit_ref, y, kx, kx_all, scale_cells, shape):
    col = place_ref[0] + y
    row = place_ref[1] + lax.broadcasted_iota(jnp.int32, shape, 0)
    wide = jnp.broadcast_to(limit_ref[0:1, :], shape)
    tall = jnp.broadcast_to(limit_ref[1:2, :], shape)
    keep = (col < wide) & ((row < tall) | (kx_all - row < tall))
    scale = jnp.where(col == 0, 1.0 / scale_cells, 2.0 / scale_cells).astype(F32)
    return jnp.where(keep, scale, 0.0)


def pick_table(geo):
    source = lax.broadcasted_iota(jnp.int32, (2 * LANES, 8 * LANES), 0) % LANES
    target = lax.broadcasted_iota(jnp.int32, (2 * LANES, 8 * LANES), 1) // LANES
    return (source == target * geo.freq).astype(BF16)


def spread_lanes(spec, y, pick_ref):
    turned = pltpu.roll(spec, LANES - y, 1)
    high, low = split(turned)
    lhs = jnp.concatenate([high, low], axis=1)
    return [mm(lhs, pick_ref[:, 2 * LANES * c : 2 * LANES * (c + 1)]) for c in range(4)]


def mix_kernel(
    place_ref, r0, r1, r2, r3, w_ref, limit_ref, width_ref, pick_ref, held_ref, mine_ref, theirs_ref, spec_ref, made, turn, laid, *, geo, block
):
    freq, kx, outs = geo.freq, geo.kx, geo.outs
    groups = spec_ref.shape[0]
    step = pl.program_id(0)
    half = groups * kx

    @pl.when(step == 0)
    def _():
        spec_ref[...] = r0[...] + r1[...] + r2[...] + r3[...]

    widths = width_ref[0:1, :] - place_ref[2]
    spec = spec_ref[...].reshape(half, LANES)
    for k in range(block):
        y = step * block + k
        re = jnp.zeros((kx, outs), F32)
        im = jnp.zeros((kx, outs), F32)
        spread = spread_lanes(spec, y, pick_ref)
        for c in range(4):
            for g in range(groups):
                i = g * 4 + c
                sr = spread[c][g * kx : (g + 1) * kx, :outs]
                si = spread[c][g * kx : (g + 1) * kx, LANES : LANES + outs]
                reads = jnp.broadcast_to(widths > i, (kx, outs))
                wr = jnp.where(reads, w_ref[i, y, 0], 0.0)
                wi = jnp.where(reads, w_ref[i, y, 1], 0.0)
                re = re + (sr * wr - si * wi)
                im = im + (sr * wi + si * wr)
        mask = limits_mask(place_ref, limit_ref, y, kx, geo.kx_all, geo.cells, (kx, outs))
        made[pl.ds(y * kx, kx), :outs] = re * mask
        made[pl.ds((freq + y) * kx, kx), :outs] = im * mask

    @pl.when(step == pl.num_programs(0) - 1)
    def _():
        place = lane_group((2 * groups, LANES), 2 * freq)
        for j in range(kx):
            slot = j % turn.shape[0]
            turn[slot, :, : 2 * freq] = made[pl.ds(j, 2 * freq, stride=kx), :].T
            line = jnp.zeros((2 * groups, LANES), F32)
            for c in range(4):
                one = turn[slot, pl.ds(c, 2 * groups, stride=4), :]
                line = jnp.where(place == c, pltpu.roll(one, 2 * freq * c, 1) if c else one, line)
            laid[pl.ds(j, 2 * groups, stride=kx), :] = line
        mine_ref[...] = laid[pl.ds(place_ref[3] * half, half), :].reshape(mine_ref.shape)
        theirs_ref[...] = laid[pl.ds((1 - place_ref[3]) * half, half), :].reshape(mine_ref.shape)


def back_kernel(place_ref, own_ref, peer_ref, w_ref, limit_ref, width_ref, held_ref, out_ref, gm_ref, made, turn, laid, *, geo, block):
    freq, kx, outs = geo.freq, geo.kx, geo.outs
    step = pl.program_id(0)
    groups = out_ref.shape[0]
    half = groups * kx
    lane = lax.broadcasted_iota(jnp.int32, (kx, LANES), 1)

    @pl.when(step == 0)
    def _():
        laid[pl.ds(place_ref[3] * half, half), :] = own_ref[...].reshape(half, LANES)
        laid[pl.ds((1 - place_ref[3]) * half, half), :] = peer_ref[...].reshape(half, LANES)
        for j in range(kx):
            slot = j % turn.shape[0]
            line = laid[pl.ds(j, 2 * groups, stride=kx), :]
            for c in range(4):
                turn[slot, pl.ds(c, 2 * groups, stride=4), :] = (
                    pltpu.roll(line, LANES - 2 * freq * c, 1) if c else line
                )
            made[pl.ds(j, 2 * freq, stride=kx), :] = turn[slot].T[: 2 * freq]
        out_ref[...] = jnp.zeros_like(out_ref)

    widths = width_ref[0:1, :] - place_ref[2]
    for k in range(block):
        y = step * block + k
        mask = limits_mask(place_ref, limit_ref, y, kx, geo.kx_all, geo.cells, (kx, outs))
        gr = made[pl.ds(y * kx, kx), :outs] * mask
        gi = made[pl.ds((freq + y) * kx, kx), :outs] * mask
        gm_ref[k, 0] = gr
        gm_ref[k, 1] = gi
        for g in range(groups):
            line = out_ref[g]
            for c in range(4):
                i = g * 4 + c
                reads = jnp.broadcast_to(widths > i, (kx, outs))
                wr = jnp.where(reads, w_ref[i, y, 0], 0.0)
                wi = jnp.where(reads, w_ref[i, y, 1], 0.0)
                br = jnp.sum(gr * wr + gi * wi, axis=1, keepdims=True)
                bi = jnp.sum(gi * wr - gr * wi, axis=1, keepdims=True)
                line = jnp.where(lane == 32 * c + y, jnp.broadcast_to(br, (kx, LANES)), line)
                line = jnp.where(lane == 32 * c + freq + y, jnp.broadcast_to(bi, (kx, LANES)), line)
            out_ref[g] = line


def outer_kernel(place_ref, spec_ref, gm_ref, width_ref, pick_ref, held_ref, out_ref, *, geo):
    kx, outs = geo.kx, geo.outs
    block = out_ref.shape[1]
    step = pl.program_id(0)
    groups = spec_ref.shape[0]
    widths = width_ref[0:1, :] - place_ref[2]
    spec = spec_ref[...].reshape(groups * kx, LANES)
    for k in range(block):
        gr = gm_ref[k, 0]
        gi = gm_ref[k, 1]
        spread = spread_lanes(spec, step * block + k, pick_ref)
        for c in range(4):
            for g in range(groups):
                i = g * 4 + c
                sr = spread[c][g * kx : (g + 1) * kx, :outs]
                si = spread[c][g * kx : (g + 1) * kx, LANES : LANES + outs]
                reads = jnp.broadcast_to(widths > i, (kx, outs))
                out_ref[i, k, 0] = jnp.where(reads, sr * gr + si * gi, 0.0)
                out_ref[i, k, 1] = jnp.where(reads, sr * gi - si * gr, 0.0)


def prefetch_kernel(after_ref, held_ref, source_ref, target_ref, sem):
    del after_ref, held_ref
    copy = pltpu.make_async_copy(source_ref, target_ref, sem)
    copy.start()
    copy.wait()


def prefetch(x, after, held):
    anywhere = pl.BlockSpec(memory_space=pl.ANY)
    return pl.pallas_call(
        prefetch_kernel,
        in_specs=[anywhere] * 3,
        out_specs=anywhere,
        out_shape=pltpu.VMEM(x.shape, x.dtype),
        scratch_shapes=[pltpu.SemaphoreType.DMA],
        compiler_params=pltpu.CompilerParams(vmem_limit_bytes=1 << 20),
        cost_estimate=cost(4),
        name="prefetch",
    )(after, resident(held), streamed(x))


class Geometry:
    def __init__(self, field, weight):
        self.channels, self.rows, self.cols = field.shape
        self.outs, self.freq, self.kx = weight.shape[1], weight.shape[2], weight.shape[4]
        self.slabs = lax.axis_size("slab")
        self.modes = lax.axis_size("mode")
        self.chans = lax.axis_size("chan")
        self.slab = lax.axis_index("slab")
        self.mode = lax.axis_index("mode")
        self.chan = lax.axis_index("chan")
        self.kx_all = self.kx * self.slabs
        self.all_rows = self.rows * self.slabs
        self.all_cols = self.cols * self.modes
        self.cells = float(self.all_rows * self.all_cols)
        self.fold = 16 * ((2 * (self.kx_all // 2 + 1) + 15) // 16)

    def fits(self):
        return (
            self.modes == 2
            and self.chans == 2
            and self.slabs == 4
            and self.freq == 16
            and self.kx_all == 64
            and self.kx % 8 == 0
            and self.channels % 8 == 0
            and self.rows % 16 == 0
            and self.cols % LANES == 0
            and 3 * self.fold <= 256
        )


def swap(x, name):
    n = lax.axis_size(name)
    return lax.ppermute(x, name, [(i, (i + 1) % n) for i in range(n)])


def fetch(x, name, distance):
    n = lax.axis_size(name)
    return lax.ppermute(x, name, [((i + distance) % n, i) for i in range(n)])


def send(x, name, distance):
    n = lax.axis_size(name)
    return lax.ppermute(x, name, [(i, (i + distance) % n) for i in range(n)])


def whole(shape):
    return pl.BlockSpec(shape, lambda *_: (0,) * len(shape))


SMEM = pl.BlockSpec(memory_space=pltpu.SMEM)


FORWARD_LIMIT = 16 << 20
MIX_LIMIT = 16 << 20
MIDDLE_LIMIT = 24 << 20
LAST_LIMIT = 24 << 20
LAST_GROUPS = 2


def cost(micros):
    return pl.CostEstimate(flops=int(micros * 1.0e8), bytes_accessed=1 << 20, transcendentals=0)


def params(limit):
    return pltpu.CompilerParams(dimension_semantics=("arbitrary",), vmem_limit_bytes=limit)


VMEM = pl.BlockSpec(memory_space=pltpu.VMEM)
ANYWHERE = pl.BlockSpec(memory_space=pl.ANY)


def streamed(x):
    return pltpu.with_memory_space_constraint(x, pltpu.HBM)


def resident(x):
    return pltpu.with_memory_space_constraint(x, pltpu.VMEM)


def reduce_spectrum(own, other, geo):
    own = own + swap(other, "mode")
    return [own[0]] + [send(own[d], "slab", d) for d in range(1, geo.slabs)]


def gather_slabs(mine, geo):
    return [mine] + [fetch(mine, "slab", d) for d in range(1, geo.slabs)]


def gather_halves(near):
    return near + [swap(piece, "mode") for piece in near]


def fast_local(
    source_field, cotangent, spectral_weight, skip_gain, channel_bias, mode_limit, width_limit, geo
):
    channels, rows, cols = source_field.shape
    groups = channels // 4
    fwd_cols, fwd_rows, inv_cols, inv_rows, fold = plan_tables(geo)
    pick = pick_table(geo)
    weight = jnp.transpose(spectral_weight, (0, 2, 3, 4, 1))
    field = source_field.shape
    field_spec = pl.BlockSpec((4, rows, cols), lambda s: (s, 0, 0))
    piece = (groups, geo.kx, LANES)
    piece_shape = jax.ShapeDtypeStruct(piece, F32)
    place = jnp.stack([geo.mode * geo.freq, geo.slab * geo.kx, geo.chan * channels, geo.chan]).astype(jnp.int32)
    limits = jnp.transpose(mode_limit)
    widths = width_limit[None, :]

    own, other, kept = pl.pallas_call(
        forward_kernel,
        grid=(groups,),
        in_specs=[SMEM, ANYWHERE, VMEM, VMEM],
        out_specs=[VMEM] * 3,
        out_shape=[jax.ShapeDtypeStruct((geo.slabs,) + piece, F32)] * 2 + [pltpu.VMEM(field, F32)],
        scratch_shapes=[pltpu.SemaphoreType.DMA((groups,))],
        compiler_params=params(FORWARD_LIMIT),
        cost_estimate=cost(6),
        name="forward",
    )(place, streamed(source_field), fwd_cols, fwd_rows)
    parts = reduce_spectrum(own, other, geo)
    near_weight = prefetch(weight, parts[0], kept)

    block = 4
    steps = geo.freq // block
    w_out = pl.BlockSpec((channels, block, 2, geo.kx, geo.outs), lambda s: (0, s, 0, 0, 0))
    g_spec = pl.BlockSpec((block, 2, geo.kx, geo.outs), lambda s: (s, 0, 0, 0))
    modes_shape = jax.ShapeDtypeStruct((geo.freq, 2, geo.kx, geo.outs), F32)
    relay = [
        pltpu.VMEM((2 * geo.freq * geo.kx, LANES), F32),
        pltpu.VMEM((4, LANES, LANES), F32),
        pltpu.VMEM((2 * groups * geo.kx, LANES), F32),
    ]
    mine, theirs, spectra = pl.pallas_call(
        functools.partial(mix_kernel, geo=geo, block=block),
        grid=(steps,),
        in_specs=[SMEM] + [VMEM] * 8 + [ANYWHERE],
        out_specs=[VMEM] * 3,
        out_shape=[piece_shape] * 3,
        scratch_shapes=relay,
        compiler_params=params(MIX_LIMIT),
        cost_estimate=cost(3),
        name="mix",
    )(place, *parts, resident(near_weight), limits, widths, pick, resident(kept))
    pieces = gather_halves(gather_slabs(mine + swap(theirs, "chan"), geo))

    wide = jax.ShapeDtypeStruct((geo.slabs, groups + 1) + piece[1:], F32)
    fields = len(pieces) + 2
    output, grad_sum, own, other = pl.pallas_call(
        functools.partial(middle_kernel, pieces=len(pieces)),
        grid=(groups,),
        in_specs=[SMEM, SMEM] + [VMEM] * (len(pieces) + 1) + [field_spec] + [VMEM] * 5,
        out_specs=[field_spec, VMEM, VMEM, VMEM],
        out_shape=[jax.ShapeDtypeStruct(field, F32), pltpu.VMEM(field, F32), wide, wide],
        scratch_shapes=[
            pltpu.VMEM((4, 256, cols), BF16),
            pltpu.VMEM((2, 2 * geo.fold, cols), F32),
            pltpu.VMEM((4, rows, cols), F32),
            pltpu.VMEM((4, rows, cols), BF16),
            pltpu.VMEM((4, rows, cols), BF16),
            pltpu.VMEM((4, rows, 2 * LANES), F32),
        ],
        input_output_aliases={fields: 1},
        compiler_params=params(MIDDLE_LIMIT),
        cost_estimate=cost(20),
        name="middle",
    )(
        skip_gain, channel_bias, *pieces, resident(kept), streamed(cotangent), fold, inv_cols, inv_rows, fwd_cols, fwd_rows
    )
    parts = reduce_spectrum(own, other, geo)
    near_weight = prefetch(weight, parts[0], grad_sum)
    grads = parts[0] + parts[1] + parts[2] + parts[3]
    sums = grads[groups]
    grads = grads[:groups]
    back, grad_modes = pl.pallas_call(
        functools.partial(back_kernel, geo=geo, block=block),
        grid=(steps,),
        in_specs=[SMEM] + [VMEM] * 5 + [ANYWHERE],
        out_specs=[VMEM, g_spec],
        out_shape=[piece_shape, modes_shape],
        scratch_shapes=relay,
        compiler_params=params(MIX_LIMIT),
        cost_estimate=cost(3),
        name="back",
    )(place, grads, swap(grads, "chan"), resident(near_weight), limits, widths, resident(grad_sum))
    near = gather_slabs(back, geo)
    spectral_grad = pl.pallas_call(
        functools.partial(outer_kernel, geo=geo),
        grid=(steps,),
        in_specs=[SMEM, VMEM, g_spec, VMEM, VMEM, ANYWHERE],
        out_specs=w_out,
        out_shape=jax.ShapeDtypeStruct(weight.shape, F32),
        compiler_params=params(MIX_LIMIT),
        cost_estimate=cost(4),
        name="outer",
    )(place, spectra, grad_modes, widths, pick, resident(grad_sum))
    near, spectral_grad = lax.optimization_barrier((near, spectral_grad))
    pieces = gather_halves(near)
    field_grad = pl.pallas_call(
        functools.partial(last_kernel, pieces=len(pieces)),
        grid=(groups // LAST_GROUPS,),
        in_specs=[SMEM] + [VMEM] * (len(pieces) + 4),
        out_specs=pl.BlockSpec((4 * LAST_GROUPS, rows, cols), lambda s: (s, 0, 0)),
        out_shape=jax.ShapeDtypeStruct(field, F32),
        compiler_params=params(LAST_LIMIT),
        cost_estimate=cost(7),
        name="last",
    )(skip_gain, *pieces, resident(grad_sum), fold, inv_cols, inv_rows)
    return (
        output,
        field_grad,
        jnp.transpose(spectral_grad, (0, 4, 1, 2, 3)),
        sums[0, :channels],
        sums[1, :channels],
    )


precise = lax.Precision.HIGHEST


def column_table(extent, freq_count, first_cell, cell_count):
    cell_index = first_cell + jnp.arange(cell_count, dtype=jnp.int32)
    wave_index = jnp.arange(freq_count, dtype=jnp.int32)
    products = (cell_index[:, None] * wave_index[None, :] % extent).astype(jnp.float32)
    angles = products * (2.0 * math.pi / extent)
    return jnp.stack([jnp.cos(angles), -jnp.sin(angles)], axis=-1).reshape(
        cell_count, 2 * freq_count
    )


def row_tables(extent, freq_count, first_cell, cell_count):
    cell_index = first_cell + jnp.arange(cell_count, dtype=jnp.int32)
    column = jnp.arange(2 * freq_count, dtype=jnp.int32)
    wave_index = column + jnp.where(column >= freq_count, extent - 2 * freq_count, 0)
    products = (cell_index[:, None] * wave_index[None, :] % extent).astype(jnp.float32)
    angles = products * (2.0 * math.pi / extent)
    return (jnp.cos(angles), jnp.sin(angles))


def row_forward(lined, row_cos, row_sin):
    line_real = lined[:, 0]
    line_imag = lined[:, 1]
    out_real = jnp.dot(line_real, row_cos, precision=precise) + jnp.dot(
        line_imag, row_sin, precision=precise
    )
    out_imag = jnp.dot(line_imag, row_cos, precision=precise) - jnp.dot(
        line_real, row_sin, precision=precise
    )
    return jnp.stack([out_real, out_imag], axis=1)


def row_inverse(modes_in, row_cos, row_sin):
    mode_real = modes_in[:, 0]
    mode_imag = modes_in[:, 1]
    back_real = jnp.dot(mode_real, row_cos.T, precision=precise) - jnp.dot(
        mode_imag, row_sin.T, precision=precise
    )
    back_imag = jnp.dot(mode_real, row_sin.T, precision=precise) + jnp.dot(
        mode_imag, row_cos.T, precision=precise
    )
    return jnp.stack([back_real, back_imag], axis=1)


def contract(spectra, weight):
    spec_real = spectra[:, :, 0]
    spec_imag = spectra[:, :, 1]
    weight_real = weight[:, :, :, 0]
    weight_imag = weight[:, :, :, 1]
    out_real = jnp.einsum("iyx,ioyx->oyx", spec_real, weight_real, precision=precise) - jnp.einsum(
        "iyx,ioyx->oyx", spec_imag, weight_imag, precision=precise
    )
    out_imag = jnp.einsum("iyx,ioyx->oyx", spec_real, weight_imag, precision=precise) + jnp.einsum(
        "iyx,ioyx->oyx", spec_imag, weight_real, precision=precise
    )
    return jnp.stack([out_real, out_imag], axis=2)


def contract_back(grads, weight):
    grad_real = grads[:, :, 0]
    grad_imag = grads[:, :, 1]
    weight_real = weight[:, :, :, 0]
    weight_imag = weight[:, :, :, 1]
    back_real = jnp.einsum("oyx,ioyx->iyx", grad_real, weight_real, precision=precise) + jnp.einsum(
        "oyx,ioyx->iyx", grad_imag, weight_imag, precision=precise
    )
    back_imag = jnp.einsum("oyx,ioyx->iyx", grad_imag, weight_real, precision=precise) - jnp.einsum(
        "oyx,ioyx->iyx", grad_real, weight_imag, precision=precise
    )
    return jnp.stack([back_real, back_imag], axis=2)


def outer_grad(spectra, grads):
    spec_real = spectra[:, :, 0]
    spec_imag = spectra[:, :, 1]
    grad_real = grads[:, :, 0]
    grad_imag = grads[:, :, 1]
    real_side = jnp.einsum("iyx,oyx->ioyx", spec_real, grad_real) + jnp.einsum(
        "iyx,oyx->ioyx", spec_imag, grad_imag
    )
    imag_side = jnp.einsum("iyx,oyx->ioyx", spec_real, grad_imag) - jnp.einsum(
        "iyx,oyx->ioyx", spec_imag, grad_real
    )
    return jnp.stack([real_side, imag_side], axis=3)


def mode_weights(limit_rows, col_freq, row_freq, kx_count, cells_total):
    keep_cols = col_freq[None, :] < limit_rows[:, 0:1]
    keep_rows = (row_freq[None, :] < limit_rows[:, 1:2]) | (
        (kx_count - row_freq)[None, :] < limit_rows[:, 1:2]
    )
    scales = jnp.where(col_freq == 0, 1.0, 2.0).astype(jnp.float32) / cells_total
    joined = keep_cols[:, :, None] & keep_rows[:, None, :]
    return (joined.astype(jnp.float32) * scales[None, :, None])[:, :, None, :]


def read_mask(in_index, width_limit):
    return (in_index[:, None] < width_limit[None, :]).astype(jnp.float32)[:, :, None, None, None]


def plain_local(
    source_field, cotangent, spectral_weight, skip_gain, channel_bias, mode_limit, width_limit
):
    channels, row_count, col_count = source_field.shape
    slab_count = lax.axis_size("slab")
    mode_count = lax.axis_size("mode")
    slab_index = lax.axis_index("slab")
    mode_index = lax.axis_index("mode")
    chan_index = lax.axis_index("chan")
    local_freq = spectral_weight.shape[2]
    local_kx = spectral_weight.shape[4]
    freq_count = local_freq * mode_count
    kx_count = local_kx * slab_count
    all_rows = row_count * slab_count
    all_cols = col_count * mode_count
    column_tab = column_table(all_cols, freq_count, mode_index * col_count, col_count)
    row_cos, row_sin = row_tables(all_rows, freq_count, slab_index * row_count, row_count)

    def spectrum(values):
        partial_cols = jnp.einsum("chw,wk->ckh", values, column_tab, precision=precise)
        summed_cols = lax.psum_scatter(partial_cols, "mode", scatter_dimension=1, tiled=True)
        paired = summed_cols.reshape(values.shape[0] * local_freq, 2, row_count)
        spectra = lax.psum_scatter(
            row_forward(paired, row_cos, row_sin), "slab", scatter_dimension=2, tiled=True
        )
        return spectra.reshape(values.shape[0], local_freq, 2, local_kx)

    def synthesis(modes_in):
        whole_modes = lax.all_gather(modes_in, "slab", axis=3, tiled=True)
        rebuilt = row_inverse(
            whole_modes.reshape(channels * local_freq, 2, kx_count), row_cos, row_sin
        )
        rebuilt = rebuilt.reshape(channels, 2 * local_freq, row_count)
        gathered = lax.all_gather(rebuilt, "mode", axis=1, tiled=True)
        return jnp.einsum("ckh,wk->chw", gathered, column_tab, precision=precise)

    in_index = chan_index * channels + jnp.arange(channels, dtype=jnp.int32)
    col_freq = mode_index * local_freq + jnp.arange(local_freq, dtype=jnp.int32)
    row_freq = slab_index * local_kx + jnp.arange(local_kx, dtype=jnp.int32)
    limit_rows = lax.dynamic_slice_in_dim(mode_limit, chan_index * channels, channels, 0)
    weights = mode_weights(limit_rows, col_freq, row_freq, kx_count, all_rows * all_cols)
    reads = read_mask(in_index, width_limit)
    masked_weight = spectral_weight * reads
    spectra = spectrum(source_field)
    out_modes = (
        lax.psum_scatter(contract(spectra, masked_weight), "chan", scatter_dimension=0, tiled=True)
        * weights
    )
    branch = synthesis(out_modes)
    skip_scale = skip_gain[:, None, None]
    summed = branch + skip_scale * source_field + channel_bias[:, None, None]
    output, gelu_back = jax.vjp(jax.nn.gelu, summed)
    grad_sum = gelu_back(cotangent)[0]
    grad_modes = spectrum(grad_sum) * weights
    all_grads = lax.all_gather(grad_modes, "chan", axis=0, tiled=True)
    spectral_grad = outer_grad(spectra, all_grads) * reads
    field_grad = synthesis(contract_back(all_grads, masked_weight)) + skip_scale * grad_sum
    gate_grad, bias_grad = lax.psum(
        (jnp.sum(grad_sum * source_field, axis=(1, 2)), jnp.sum(grad_sum, axis=(1, 2))),
        ("slab", "mode"),
    )
    return (output, field_grad, spectral_grad, gate_grad, bias_grad)


def local(*args):
    geo = Geometry(args[0], args[2])
    if geo.fits():
        return fast_local(*args, geo)
    return plain_local(*args)


def solution(mesh):
    in_specs = (
        P(("member", "chan"), "slab", "mode"),
        P(("member", "chan"), "slab", "mode"),
        P(("member", "chan"), None, "mode", None, "slab"),
        P(("member", "chan")),
        P(("member", "chan")),
        P("member", None),
        P("member"),
    )
    out_specs = (
        P(("member", "chan"), "slab", "mode"),
        P(("member", "chan"), "slab", "mode"),
        P(("member", "chan"), None, "mode", None, "slab"),
        P(("member", "chan")),
        P(("member", "chan")),
    )
    return jax.shard_map(local, mesh=mesh, in_specs=in_specs, out_specs=out_specs, check_vma=False)
```

```python
import functools
import math

import jax
import jax.numpy as jnp
from jax import lax
from jax.experimental import pallas as pl
from jax.experimental.pallas import tpu as pltpu
from jax.sharding import PartitionSpec as P

F32 = jnp.float32
BF16 = jnp.bfloat16
LANES = 128
GELU_A = math.sqrt(2.0 / math.pi)
GELU_B = GELU_A * 0.044715


def split(x):
    high = x.astype(BF16)
    return high, (x - high.astype(F32)).astype(BF16)


def split_table(x):
    high = lax.reduce_precision(x, 8, 7)
    return high.astype(BF16), (x - high).astype(BF16)


def mm(a, b):
    return jnp.dot(a, b, preferred_element_type=F32)


def angles(cells, freqs, extent):
    products = (cells[:, None] * freqs[None, :] % extent).astype(F32)
    return products * (2.0 * math.pi / extent)


def plan_tables(geo):
    col_cell = geo.mode * geo.cols + jnp.arange(geo.cols, dtype=jnp.int32)
    rel_mode = (geo.mode + jnp.arange(geo.modes, dtype=jnp.int32)) % geo.modes
    freq = (rel_mode[:, None] * geo.freq + jnp.arange(geo.freq, dtype=jnp.int32)[None, :])
    theta = angles(col_cell, freq.reshape(-1), geo.all_cols).reshape(geo.cols, geo.modes, geo.freq)
    cos, sin = jnp.cos(theta), jnp.sin(theta)
    first = jnp.stack([cos, -sin], axis=2).reshape(geo.cols, -1)
    second = jnp.stack([-sin, -cos], axis=2).reshape(geo.cols, -1)
    first_h, first_l = split_table(first)
    second_h, second_l = split_table(second)
    forward_cols = jnp.concatenate([first_h, first_l], axis=1)
    inverse_cols = jnp.stack(
        [
            jnp.concatenate([high.T, high.T, low.T, low.T], axis=0)
            for high, low in ((first_h, first_l), (second_h, second_l))
        ]
    )
    row_cell = geo.slab * geo.rows + jnp.arange(geo.rows, dtype=jnp.int32)
    rel_slab = (geo.slab + jnp.arange(geo.slabs, dtype=jnp.int32)) % geo.slabs
    place = (rel_slab[:, None] * geo.kx + jnp.arange(geo.kx, dtype=jnp.int32)[None, :]).reshape(-1)
    half = geo.slabs * geo.kx // 2
    wave = jnp.where(place < half, place, place - 2 * half)
    theta = angles(wave % geo.all_rows, row_cell, geo.all_rows)
    forward_h, forward_l = split_table(jnp.concatenate([jnp.cos(theta), jnp.sin(theta)], axis=0))
    forward_rows = jnp.concatenate([forward_h, forward_l], axis=0)
    kept = jnp.arange(geo.fold // 2, dtype=jnp.int32)
    theta = angles(row_cell, kept, geo.all_rows)
    live = (kept <= half)[None, :]
    inverse_h, inverse_l = split_table(
        jnp.concatenate(
            [jnp.where(live, jnp.cos(theta), 0.0), jnp.where(live, jnp.sin(theta), 0.0)], axis=1
        )
    )
    rest = jnp.zeros((geo.rows, 256 - 3 * geo.fold), BF16)
    inverse_rows = jnp.concatenate([inverse_h, inverse_h, inverse_l, rest], axis=1)
    same = (jnp.abs(wave)[None, :] == kept[:, None]).astype(F32)
    fold = jnp.concatenate([same, same * jnp.sign(wave).astype(F32)[None, :]], axis=0).astype(BF16)
    return forward_cols, forward_rows, inverse_cols, inverse_rows, jnp.concatenate([fold, fold], axis=1)


def lane_group(shape, width):
    return lax.broadcasted_iota(jnp.int32, shape, 1) // width


def pair_spectra(first, second, row_tab, freq):
    sides = row_tab.shape[0] // 2
    high, low = split(jnp.concatenate([first, second], axis=1))
    both = mm(row_tab, high)
    total = both[:sides] + both[sides:] + mm(row_tab[:sides], low)
    out = []
    for lane in (0, LANES):
        one = total[:, lane : lane + LANES]
        one = one + pltpu.roll(one, 64, 1)
        cos, sin = one[: sides // 2], one[sides // 2 :]
        real = lane_group(sin.shape, freq) % 2 == 0
        out.append(cos + jnp.where(real, pltpu.roll(sin, LANES - freq, 1), -pltpu.roll(sin, freq, 1)))
    return out


def write_spectra(doubled, own_ref, other_ref, group):
    turned = [pltpu.roll(s, 32, 1) for s in doubled]
    place = lane_group(doubled[0].shape, 32)

    def weave(arrays):
        return jnp.where(
            place == 0,
            arrays[0],
            jnp.where(place == 1, arrays[1], jnp.where(place == 2, arrays[2], arrays[3])),
        )

    own = weave([doubled[0], turned[1], doubled[2], turned[3]])
    other = weave([turned[0], doubled[1], turned[2], doubled[3]])
    slabs, _, kx, _ = own_ref.shape
    for q in range(slabs):
        own_ref[q, group] = own[q * kx : (q + 1) * kx]
        other_ref[q, group] = other[q * kx : (q + 1) * kx]


def emitting(part_ref, row_ref, own_ref, other_ref, at, freq):
    held = {}

    def pair(k):
        held[k] = pair_spectra(part_ref[2 * k], part_ref[2 * k + 1], row_ref[...], freq)

    def write():
        write_spectra(held[0] + held[1], own_ref, other_ref, at)

    return [functools.partial(pair, 0), functools.partial(pair, 1), write]


def forward_kernel(place_ref, x_ref, col_ref, row_ref, own_ref, other_ref, keep_ref, sems, part_ref, *, freq):
    del place_ref
    step = pl.program_id(0)

    def fetching(at):
        four = pl.ds(at * 4, 4)
        return pltpu.make_async_copy(x_ref.at[four], keep_ref.at[four], sems.at[at])

    @pl.when(step == 0)
    def _():
        for at in range(FORWARD_AHEAD):
            fetching(at).start()

    @pl.when(step + FORWARD_AHEAD < pl.num_programs(0))
    def _():
        fetching(step + FORWARD_AHEAD).start()

    @pl.when(step == 0)
    def _():
        part_ref[...] = jnp.zeros_like(part_ref)

    fetching(step).wait()
    emits = emitting(part_ref, row_ref, own_ref, other_ref, jnp.maximum(step - 1, 0), freq)
    for c in range(4):
        if c < len(emits):
            emits[c]()
        high, low = split(keep_ref[step * 4 + c])
        part_ref[c] = mm(high, col_ref[...]) + mm(low, col_ref[...])

    @pl.when(step == pl.num_programs(0) - 1)
    def _():
        for task in emitting(part_ref, row_ref, own_ref, other_ref, step, freq):
            task()


def fold_modes(piece_refs, step, fold_ref):
    slabs = len(piece_refs) // 2
    halves = [
        jnp.concatenate([r[step] for r in piece_refs[m * slabs : (m + 1) * slabs]], axis=0) for m in (0, 1)
    ]
    high, low = split(jnp.concatenate(halves, axis=1))
    return mm(fold_ref[...], jnp.concatenate([high, low], axis=0))


def line_up(folded, c):
    group = lane_group((folded.shape[0], LANES), 32)
    a, b = folded[:, :LANES], folded[:, LANES:]
    a_at = [a if (t - c) % 4 == 0 else pltpu.roll(a, 32 * ((t - c) % 4), 1) for t in (0, 2)]
    b_at = [b if (t - c) % 4 == 0 else pltpu.roll(b, 32 * ((t - c) % 4), 1) for t in (1, 3)]
    one = jnp.where(
        group == 0, a_at[0], jnp.where(group == 1, b_at[0], jnp.where(group == 2, a_at[1], b_at[1]))
    )
    top = one.astype(BF16).astype(F32)
    return jnp.where(group < 2, top, one - top)


def spread_columns(rows, side, inv_col_ref):
    half = rows[0].shape[0] // 2
    lhs = jnp.concatenate([r[side * half : (side + 1) * half] for r in rows], axis=0).astype(BF16)
    return mm(jnp.concatenate([lhs, lhs], axis=1), inv_col_ref[side])


def stack_operand(plus, minus, add=None):
    if add is not None:
        plus = plus + jnp.where(lax.broadcasted_iota(jnp.int32, plus.shape, 0) == 0, add, 0.0)
    high, low = split(jnp.concatenate([plus, minus], axis=0))
    rest = jnp.zeros((256 - 3 * high.shape[0], high.shape[1]), BF16)
    return jnp.concatenate([high, low, high, rest], axis=0)


def preparing(piece_refs, at, fold_ref, inv_col_ref, wide_ref, ready, biases):
    held = {}
    half = fold_ref.shape[0] // 2

    def begin():
        held["folded"] = fold_modes(piece_refs, at, fold_ref)

    def line(c):
        held[c] = line_up(held["folded"], c)

    def spread(side):
        wide_ref[side] = spread_columns([held[c] for c in range(4)], side, inv_col_ref)

    def stack(c):
        plus, minus = (wide_ref[side, c * half : (c + 1) * half] for side in (0, 1))
        ready[c] = stack_operand(plus, minus, None if biases is None else biases[c])

    early = [begin] + [functools.partial(line, c) for c in range(4)]
    early += [functools.partial(spread, side) for side in (0, 1)]
    return early, [functools.partial(stack, c) for c in range(4)]


CHUNK = 16


def middle_kernel(place_ref, skip_ref, bias_ref, *refs, pieces, freq):
    piece_refs = refs[:pieces]
    x_ref, ct_ref, fold_ref, inv_col_ref, inv_row_ref, col_ref, row_ref = refs[pieces : pieces + 7]
    out_ref, gs_ref, own_ref, other_ref, ready, wide_ref, branch, high_ref, low_ref, part_ref = refs[pieces + 7 :]
    step = pl.program_id(0)
    last = pl.num_programs(0) - 1
    rows, cols = x_ref.shape[1:]
    sums = own_ref.shape[1] - 1

    def prepare_group(at):
        biases = [bias_ref[at * 4 + c] for c in range(4)]
        return preparing(piece_refs, at, fold_ref, inv_col_ref, wide_ref, ready, biases)

    def emit_group(at):
        return emitting(part_ref, row_ref, own_ref, other_ref, at, freq)

    @pl.when(step == 0)
    def _():
        early, late = prepare_group(0)
        for task in early + late:
            task()
        part_ref[...] = jnp.zeros_like(part_ref)
        own_ref[0, sums] = jnp.zeros(own_ref.shape[2:], F32)

    early, late = prepare_group(jnp.minimum(step + 1, last))
    emits = emit_group(jnp.maximum(step - 1, 0))
    chunks = rows // CHUNK
    plan = {(0, 1): emits[0], (0, 5): emits[1], (0, 10): emits[2]}
    for k, task in enumerate(early):
        plan[(1 + k // 4, 2 + 3 * (k % 4))] = task
    for k, task in enumerate(late):
        plan[(3, 2 + 3 * k)] = task
    tile = own_ref[0, sums]
    row = lax.broadcasted_iota(jnp.int32, tile.shape, 0)
    lane = lax.broadcasted_iota(jnp.int32, tile.shape, 1)
    branch[0] = mm(inv_row_ref[...], ready[0])
    for c in range(4):
        channel = step * 4 + c
        skip = skip_ref[channel]
        gate = jnp.zeros((CHUNK, cols), F32)
        for k in range(chunks):
            r = k * CHUNK
            if (c, k) in plan:
                plan[(c, k)]()
            if k == 0 and c < 3:
                branch[c + 1] = mm(inv_row_ref[...], ready[c + 1])
            if k == 1 and c > 0:
                part_ref[c - 1] = mm(high_ref[c - 1], col_ref[...]) + mm(low_ref[c - 1], col_ref[...])
            x = x_ref[channel, r : r + CHUNK]
            v = branch[c, r : r + CHUNK] + skip * x
            q = v * v
            t = jnp.tanh(v * (q * GELU_B + GELU_A))
            s = 0.5 * t + 0.5
            out = v * s
            out_ref[c, r : r + CHUNK] = out
            slope = s + out * (1.0 - s) * (q * (6.0 * GELU_B) + 2.0 * GELU_A)
            grad = ct_ref[c, r : r + CHUNK] * slope
            gs_ref[channel, r : r + CHUNK] = grad
            gate = gate + grad * x
            top = grad.astype(BF16)
            high_ref[c, r : r + CHUNK] = top
            low_ref[c, r : r + CHUNK] = (grad - top.astype(F32)).astype(BF16)
        line = jnp.sum(gate, axis=0, keepdims=True)
        value = jnp.sum(sum(line[:, k : k + LANES] for k in range(0, cols, LANES)), axis=1, keepdims=True)
        tile = jnp.where((row == 0) & (lane == channel), jnp.broadcast_to(value, tile.shape), tile)
    part_ref[3] = mm(high_ref[3], col_ref[...]) + mm(low_ref[3], col_ref[...])
    own_ref[0, sums] = tile

    @pl.when(step == last)
    def _():
        for task in emit_group(last):
            task()
        whole_sums = tile
        for g in range(sums):
            lines = [ref[place_ref[4], g][0:1, :] for ref in (own_ref, other_ref)]
            line = jnp.where(place_ref[0] == 0, lines[0], lines[1])
            for c in range(4):
                value = jnp.broadcast_to(line[:, 2 * freq * c : 2 * freq * c + 1], tile.shape)
                whole_sums = jnp.where((row == 1) & (lane == g * 4 + c), value, whole_sums)
        for q in range(own_ref.shape[0]):
            own_ref[q, sums] = whole_sums
            other_ref[q, sums] = whole_sums


def last_kernel(skip_ref, *refs, pieces):
    piece_refs = refs[:pieces]
    gs_ref, fold_ref, inv_col_ref, inv_row_ref, out_ref, made_ref, sems, ready, wide_ref = refs[pieces:]
    step = pl.program_id(0)
    last = pl.num_programs(0) - 1

    def storing(at):
        four = pl.ds(at * 4, 4)
        return pltpu.make_async_copy(made_ref.at[four], out_ref.at[four], sems.at[at])

    def prepare_group(at):
        return preparing(piece_refs, at, fold_ref, inv_col_ref, wide_ref, ready, None)

    @pl.when(step == 0)
    def _():
        early, late = prepare_group(0)
        for task in early + late:
            task()

    early, late = prepare_group(jnp.minimum(step + 1, last))
    turns = [early[:1], early[1:5], early[5:], []]
    for c in range(4):
        channel = step * 4 + c
        made_ref[channel] = mm(inv_row_ref[...], ready[c]) + skip_ref[channel] * gs_ref[channel]
        for task in turns[c]:
            task()
    for task in late:
        task()
    storing(step).start()

    @pl.when(step == last)
    def _():
        for at in range(sems.shape[0]):
            storing(at).wait()


def limits_mask(place_ref, limit_ref, y, kx, kx_all, scale_cells, shape):
    col = place_ref[0] + y
    row = place_ref[1] + lax.broadcasted_iota(jnp.int32, shape, 0)
    wide = jnp.broadcast_to(limit_ref[0:1, :], shape)
    tall = jnp.broadcast_to(limit_ref[1:2, :], shape)
    keep = (col < wide) & ((row < tall) | (kx_all - row < tall))
    scale = jnp.where(col == 0, 1.0 / scale_cells, 2.0 / scale_cells).astype(F32)
    return jnp.where(keep, scale, 0.0)


def pick_table(geo):
    source = lax.broadcasted_iota(jnp.int32, (2 * LANES, 8 * LANES), 0) % LANES
    target = lax.broadcasted_iota(jnp.int32, (2 * LANES, 8 * LANES), 1) // LANES
    return (source == target * geo.freq).astype(BF16)


def spread_lanes(spec, y, pick_ref):
    turned = pltpu.roll(spec, LANES - y, 1)
    high, low = split(turned)
    lhs = jnp.concatenate([high, low], axis=1)
    return [mm(lhs, pick_ref[:, 2 * LANES * c : 2 * LANES * (c + 1)]) for c in range(4)]


def mix_kernel(
    place_ref, r0, r1, r2, r3, w_ref, limit_ref, width_ref, pick_ref, held_ref, mine_ref, theirs_ref, spec_ref, made, turn, laid, *, geo, block
):
    freq, kx, outs = geo.freq, geo.kx, geo.outs
    groups = spec_ref.shape[0]
    step = pl.program_id(0)
    half = groups * kx

    @pl.when(step == 0)
    def _():
        spec_ref[...] = r0[...] + r1[...] + r2[...] + r3[...]

    widths = width_ref[0:1, :] - place_ref[2]
    spec = spec_ref[...].reshape(half, LANES)
    for k in range(block):
        y = step * block + k
        re = jnp.zeros((kx, outs), F32)
        im = jnp.zeros((kx, outs), F32)
        spread = spread_lanes(spec, y, pick_ref)
        for c in range(4):
            for g in range(groups):
                i = g * 4 + c
                sr = spread[c][g * kx : (g + 1) * kx, :outs]
                si = spread[c][g * kx : (g + 1) * kx, LANES : LANES + outs]
                reads = jnp.broadcast_to(widths > i, (kx, outs))
                wr = jnp.where(reads, w_ref[i, y, 0], 0.0)
                wi = jnp.where(reads, w_ref[i, y, 1], 0.0)
                re = re + (sr * wr - si * wi)
                im = im + (sr * wi + si * wr)
        mask = limits_mask(place_ref, limit_ref, y, kx, geo.kx_all, geo.cells, (kx, outs))
        made[pl.ds(y * kx, kx), :outs] = re * mask
        made[pl.ds((freq + y) * kx, kx), :outs] = im * mask

    @pl.when(step == pl.num_programs(0) - 1)
    def _():
        place = lane_group((2 * groups, LANES), 2 * freq)
        for j in range(kx):
            slot = j % turn.shape[0]
            turn[slot, :, : 2 * freq] = made[pl.ds(j, 2 * freq, stride=kx), :].T
            line = jnp.zeros((2 * groups, LANES), F32)
            for c in range(4):
                one = turn[slot, pl.ds(c, 2 * groups, stride=4), :]
                line = jnp.where(place == c, pltpu.roll(one, 2 * freq * c, 1) if c else one, line)
            laid[pl.ds(j, 2 * groups, stride=kx), :] = line
        mine_ref[...] = laid[pl.ds(place_ref[3] * half, half), :].reshape(mine_ref.shape)
        theirs_ref[...] = laid[pl.ds((1 - place_ref[3]) * half, half), :].reshape(mine_ref.shape)


def back_kernel(place_ref, own_ref, peer_ref, w_ref, limit_ref, width_ref, held_ref, out_ref, gm_ref, made, turn, laid, *, geo, block):
    freq, kx, outs = geo.freq, geo.kx, geo.outs
    step = pl.program_id(0)
    groups = out_ref.shape[0]
    half = groups * kx
    lane = lax.broadcasted_iota(jnp.int32, (kx, LANES), 1)

    @pl.when(step == 0)
    def _():
        laid[pl.ds(place_ref[3] * half, half), :] = own_ref[...].reshape(half, LANES)
        laid[pl.ds((1 - place_ref[3]) * half, half), :] = peer_ref[...].reshape(half, LANES)
        for j in range(kx):
            slot = j % turn.shape[0]
            line = laid[pl.ds(j, 2 * groups, stride=kx), :]
            for c in range(4):
                turn[slot, pl.ds(c, 2 * groups, stride=4), :] = (
                    pltpu.roll(line, LANES - 2 * freq * c, 1) if c else line
                )
            made[pl.ds(j, 2 * freq, stride=kx), :] = turn[slot].T[: 2 * freq]
        out_ref[...] = jnp.zeros_like(out_ref)

    widths = width_ref[0:1, :] - place_ref[2]
    for k in range(block):
        y = step * block + k
        mask = limits_mask(place_ref, limit_ref, y, kx, geo.kx_all, geo.cells, (kx, outs))
        gr = made[pl.ds(y * kx, kx), :outs] * mask
        gi = made[pl.ds((freq + y) * kx, kx), :outs] * mask
        gm_ref[k, 0] = gr
        gm_ref[k, 1] = gi
        for g in range(groups):
            line = out_ref[g]
            for c in range(4):
                i = g * 4 + c
                reads = jnp.broadcast_to(widths > i, (kx, outs))
                wr = jnp.where(reads, w_ref[i, y, 0], 0.0)
                wi = jnp.where(reads, w_ref[i, y, 1], 0.0)
                br = jnp.sum(gr * wr + gi * wi, axis=1, keepdims=True)
                bi = jnp.sum(gi * wr - gr * wi, axis=1, keepdims=True)
                line = jnp.where(lane == 32 * c + y, jnp.broadcast_to(br, (kx, LANES)), line)
                line = jnp.where(lane == 32 * c + freq + y, jnp.broadcast_to(bi, (kx, LANES)), line)
            out_ref[g] = line


def outer_kernel(place_ref, spec_ref, gm_ref, width_ref, pick_ref, held_ref, out_ref, *, geo):
    kx, outs = geo.kx, geo.outs
    block = out_ref.shape[1]
    step = pl.program_id(0)
    groups = spec_ref.shape[0]
    widths = width_ref[0:1, :] - place_ref[2]
    spec = spec_ref[...].reshape(groups * kx, LANES)
    for k in range(block):
        gr = gm_ref[k, 0]
        gi = gm_ref[k, 1]
        spread = spread_lanes(spec, step * block + k, pick_ref)
        for c in range(4):
            for g in range(groups):
                i = g * 4 + c
                sr = spread[c][g * kx : (g + 1) * kx, :outs]
                si = spread[c][g * kx : (g + 1) * kx, LANES : LANES + outs]
                reads = jnp.broadcast_to(widths > i, (kx, outs))
                out_ref[i, k, 0] = jnp.where(reads, sr * gr + si * gi, 0.0)
                out_ref[i, k, 1] = jnp.where(reads, sr * gi - si * gr, 0.0)


def prefetch_kernel(after_ref, held_ref, source_ref, target_ref, sem):
    del after_ref, held_ref
    copy = pltpu.make_async_copy(source_ref, target_ref, sem)
    copy.start()
    copy.wait()


def prefetch(x, after, held):
    anywhere = pl.BlockSpec(memory_space=pl.ANY)
    return pl.pallas_call(
        prefetch_kernel,
        in_specs=[anywhere] * 3,
        out_specs=anywhere,
        out_shape=pltpu.VMEM(x.shape, x.dtype),
        scratch_shapes=[pltpu.SemaphoreType.DMA],
        compiler_params=pltpu.CompilerParams(vmem_limit_bytes=1 << 20),
        cost_estimate=cost(4),
        name="prefetch",
    )(after, resident(held), streamed(x))


class Geometry:
    def __init__(self, field, weight):
        self.channels, self.rows, self.cols = field.shape
        self.outs, self.freq, self.kx = weight.shape[1], weight.shape[2], weight.shape[4]
        self.slabs = lax.axis_size("slab")
        self.modes = lax.axis_size("mode")
        self.chans = lax.axis_size("chan")
        self.slab = lax.axis_index("slab")
        self.mode = lax.axis_index("mode")
        self.chan = lax.axis_index("chan")
        self.kx_all = self.kx * self.slabs
        self.all_rows = self.rows * self.slabs
        self.all_cols = self.cols * self.modes
        self.cells = float(self.all_rows * self.all_cols)
        self.fold = 16 * ((2 * (self.kx_all // 2 + 1) + 15) // 16)

    def fits(self):
        return (
            self.modes == 2
            and self.chans == 2
            and self.slabs == 4
            and self.freq == 16
            and self.kx_all == 64
            and self.kx % 8 == 0
            and self.channels % 4 == 0
            and self.channels <= LANES
            and self.rows % 16 == 0
            and self.cols % LANES == 0
            and 3 * self.fold <= 256
        )


def swap(x, name):
    n = lax.axis_size(name)
    return lax.ppermute(x, name, [(i, (i + 1) % n) for i in range(n)])


def fetch(x, name, distance):
    n = lax.axis_size(name)
    return lax.ppermute(x, name, [((i + distance) % n, i) for i in range(n)])


def send(x, name, distance):
    n = lax.axis_size(name)
    return lax.ppermute(x, name, [(i, (i + distance) % n) for i in range(n)])


def whole(shape):
    return pl.BlockSpec(shape, lambda *_: (0,) * len(shape))


SMEM = pl.BlockSpec(memory_space=pltpu.SMEM)


FORWARD_LIMIT = 16 << 20
FORWARD_AHEAD = 2
MIX_LIMIT = 16 << 20
MIDDLE_LIMIT = 24 << 20
LAST_LIMIT = 28 << 20


def cost(micros):
    return pl.CostEstimate(flops=int(micros * 1.0e8), bytes_accessed=1 << 20, transcendentals=0)


def params(limit):
    return pltpu.CompilerParams(dimension_semantics=("arbitrary",), vmem_limit_bytes=limit)


VMEM = pl.BlockSpec(memory_space=pltpu.VMEM)
ANYWHERE = pl.BlockSpec(memory_space=pl.ANY)


def streamed(x):
    return pltpu.with_memory_space_constraint(x, pltpu.HBM)


def resident(x):
    return pltpu.with_memory_space_constraint(x, pltpu.VMEM)


def reduce_spectrum(own, other, geo):
    own = own + swap(other, "mode")
    return [own[0]] + [send(own[d], "slab", d) for d in range(1, geo.slabs)]


def gather_slabs(mine, geo):
    return [mine] + [fetch(mine, "slab", d) for d in range(1, geo.slabs)]


def gather_halves(near):
    return near + [swap(piece, "mode") for piece in near]


def fast_local(
    source_field, cotangent, spectral_weight, skip_gain, channel_bias, mode_limit, width_limit, geo
):
    channels, rows, cols = source_field.shape
    groups = channels // 4
    fwd_cols, fwd_rows, inv_cols, inv_rows, fold = plan_tables(geo)
    pick = pick_table(geo)
    weight = jnp.transpose(spectral_weight, (0, 2, 3, 4, 1))
    field = source_field.shape
    field_spec = pl.BlockSpec((4, rows, cols), lambda s: (s, 0, 0))
    piece = (groups, geo.kx, LANES)
    piece_shape = jax.ShapeDtypeStruct(piece, F32)
    place = jnp.stack([geo.mode * geo.freq, geo.slab * geo.kx, geo.chan * channels, geo.chan, -geo.slab % geo.slabs]).astype(jnp.int32)
    limits = jnp.transpose(mode_limit)
    widths = width_limit[None, :]

    own, other, kept = pl.pallas_call(
        functools.partial(forward_kernel, freq=geo.freq),
        grid=(groups,),
        in_specs=[SMEM, ANYWHERE, VMEM, VMEM],
        out_specs=[VMEM] * 3,
        out_shape=[jax.ShapeDtypeStruct((geo.slabs,) + piece, F32)] * 2 + [pltpu.VMEM(field, F32)],
        scratch_shapes=[pltpu.SemaphoreType.DMA((groups,)), pltpu.VMEM((4, rows, LANES), F32)],
        compiler_params=params(FORWARD_LIMIT),
        cost_estimate=cost(6),
        name="forward",
    )(place, streamed(source_field), fwd_cols, fwd_rows)
    parts = reduce_spectrum(own, other, geo)
    near_weight = prefetch(weight, parts[0], kept)

    block = 4
    steps = geo.freq // block
    w_out = pl.BlockSpec((channels, block, 2, geo.kx, geo.outs), lambda s: (0, s, 0, 0, 0))
    g_spec = pl.BlockSpec((block, 2, geo.kx, geo.outs), lambda s: (s, 0, 0, 0))
    modes_shape = jax.ShapeDtypeStruct((geo.freq, 2, geo.kx, geo.outs), F32)
    relay = [
        pltpu.VMEM((2 * geo.freq * geo.kx, LANES), F32),
        pltpu.VMEM((4, LANES, LANES), F32),
        pltpu.VMEM((2 * groups * geo.kx, LANES), F32),
    ]
    mine, theirs, spectra = pl.pallas_call(
        functools.partial(mix_kernel, geo=geo, block=block),
        grid=(steps,),
        in_specs=[SMEM] + [VMEM] * 8 + [ANYWHERE],
        out_specs=[VMEM] * 3,
        out_shape=[piece_shape] * 3,
        scratch_shapes=relay,
        compiler_params=params(MIX_LIMIT),
        cost_estimate=cost(3),
        name="mix",
    )(place, *parts, resident(near_weight), limits, widths, pick, resident(kept))
    pieces = gather_halves(gather_slabs(mine + swap(theirs, "chan"), geo))

    wide = jax.ShapeDtypeStruct((geo.slabs, groups + 1) + piece[1:], F32)
    fields = len(pieces) + 3
    output, grad_sum, own, other = pl.pallas_call(
        functools.partial(middle_kernel, pieces=len(pieces), freq=geo.freq),
        grid=(groups,),
        in_specs=[SMEM] * 3 + [VMEM] * (len(pieces) + 1) + [field_spec] + [VMEM] * 5,
        out_specs=[field_spec, VMEM, VMEM, VMEM],
        out_shape=[jax.ShapeDtypeStruct(field, F32), pltpu.VMEM(field, F32), wide, wide],
        scratch_shapes=[
            pltpu.VMEM((4, 256, cols), BF16),
            pltpu.VMEM((2, 2 * geo.fold, cols), F32),
            pltpu.VMEM((4, rows, cols), F32),
            pltpu.VMEM((4, rows, cols), BF16),
            pltpu.VMEM((4, rows, cols), BF16),
            pltpu.VMEM((4, rows, LANES), F32),
        ],
        input_output_aliases={fields: 1},
        compiler_params=params(MIDDLE_LIMIT),
        cost_estimate=cost(20),
        name="middle",
    )(
        place, skip_gain, channel_bias, *pieces, resident(kept), streamed(cotangent), fold, inv_cols, inv_rows, fwd_cols, fwd_rows
    )
    parts = reduce_spectrum(own, other, geo)
    near_weight = prefetch(weight, parts[0], grad_sum)
    parts, near_weight = lax.optimization_barrier((parts, near_weight))
    grads = parts[0] + parts[1] + parts[2] + parts[3]
    sums = grads[groups]
    grads = grads[:groups]
    back, grad_modes = pl.pallas_call(
        functools.partial(back_kernel, geo=geo, block=block),
        grid=(steps,),
        in_specs=[SMEM] + [VMEM] * 5 + [ANYWHERE],
        out_specs=[VMEM, g_spec],
        out_shape=[piece_shape, modes_shape],
        scratch_shapes=relay,
        compiler_params=params(MIX_LIMIT),
        cost_estimate=cost(3),
        name="back",
    )(place, grads, swap(grads, "chan"), resident(near_weight), limits, widths, resident(grad_sum))
    near = gather_slabs(back, geo)
    spectral_grad = pl.pallas_call(
        functools.partial(outer_kernel, geo=geo),
        grid=(steps,),
        in_specs=[SMEM, VMEM, g_spec, VMEM, VMEM, ANYWHERE],
        out_specs=w_out,
        out_shape=jax.ShapeDtypeStruct(weight.shape, F32),
        compiler_params=params(MIX_LIMIT),
        cost_estimate=cost(4),
        name="outer",
    )(place, spectra, grad_modes, widths, pick, resident(grad_sum))
    near, spectral_grad = lax.optimization_barrier((near, spectral_grad))
    pieces = gather_halves(near)
    field_grad = pl.pallas_call(
        functools.partial(last_kernel, pieces=len(pieces)),
        grid=(groups,),
        in_specs=[SMEM] + [VMEM] * (len(pieces) + 4),
        out_specs=ANYWHERE,
        out_shape=jax.ShapeDtypeStruct(field, F32),
        scratch_shapes=[
            pltpu.VMEM(field, F32),
            pltpu.SemaphoreType.DMA((groups,)),
            pltpu.VMEM((4, 256, cols), BF16),
            pltpu.VMEM((2, 2 * geo.fold, cols), F32),
        ],
        compiler_params=params(LAST_LIMIT),
        cost_estimate=cost(7),
        name="last",
    )(skip_gain, *pieces, resident(grad_sum), fold, inv_cols, inv_rows)
    return (
        output,
        field_grad,
        jnp.transpose(spectral_grad, (0, 4, 1, 2, 3)),
        sums[0, :channels],
        sums[1, :channels],
    )


precise = lax.Precision.HIGHEST


def column_table(extent, freq_count, first_cell, cell_count):
    cell_index = first_cell + jnp.arange(cell_count, dtype=jnp.int32)
    wave_index = jnp.arange(freq_count, dtype=jnp.int32)
    products = (cell_index[:, None] * wave_index[None, :] % extent).astype(jnp.float32)
    angles = products * (2.0 * math.pi / extent)
    return jnp.stack([jnp.cos(angles), -jnp.sin(angles)], axis=-1).reshape(
        cell_count, 2 * freq_count
    )


def row_tables(extent, freq_count, first_cell, cell_count):
    cell_index = first_cell + jnp.arange(cell_count, dtype=jnp.int32)
    column = jnp.arange(2 * freq_count, dtype=jnp.int32)
    wave_index = column + jnp.where(column >= freq_count, extent - 2 * freq_count, 0)
    products = (cell_index[:, None] * wave_index[None, :] % extent).astype(jnp.float32)
    angles = products * (2.0 * math.pi / extent)
    return (jnp.cos(angles), jnp.sin(angles))


def row_forward(lined, row_cos, row_sin):
    line_real = lined[:, 0]
    line_imag = lined[:, 1]
    out_real = jnp.dot(line_real, row_cos, precision=precise) + jnp.dot(
        line_imag, row_sin, precision=precise
    )
    out_imag = jnp.dot(line_imag, row_cos, precision=precise) - jnp.dot(
        line_real, row_sin, precision=precise
    )
    return jnp.stack([out_real, out_imag], axis=1)


def row_inverse(modes_in, row_cos, row_sin):
    mode_real = modes_in[:, 0]
    mode_imag = modes_in[:, 1]
    back_real = jnp.dot(mode_real, row_cos.T, precision=precise) - jnp.dot(
        mode_imag, row_sin.T, precision=precise
    )
    back_imag = jnp.dot(mode_real, row_sin.T, precision=precise) + jnp.dot(
        mode_imag, row_cos.T, precision=precise
    )
    return jnp.stack([back_real, back_imag], axis=1)


def contract(spectra, weight):
    spec_real = spectra[:, :, 0]
    spec_imag = spectra[:, :, 1]
    weight_real = weight[:, :, :, 0]
    weight_imag = weight[:, :, :, 1]
    out_real = jnp.einsum("iyx,ioyx->oyx", spec_real, weight_real, precision=precise) - jnp.einsum(
        "iyx,ioyx->oyx", spec_imag, weight_imag, precision=precise
    )
    out_imag = jnp.einsum("iyx,ioyx->oyx", spec_real, weight_imag, precision=precise) + jnp.einsum(
        "iyx,ioyx->oyx", spec_imag, weight_real, precision=precise
    )
    return jnp.stack([out_real, out_imag], axis=2)


def contract_back(grads, weight):
    grad_real = grads[:, :, 0]
    grad_imag = grads[:, :, 1]
    weight_real = weight[:, :, :, 0]
    weight_imag = weight[:, :, :, 1]
    back_real = jnp.einsum("oyx,ioyx->iyx", grad_real, weight_real, precision=precise) + jnp.einsum(
        "oyx,ioyx->iyx", grad_imag, weight_imag, precision=precise
    )
    back_imag = jnp.einsum("oyx,ioyx->iyx", grad_imag, weight_real, precision=precise) - jnp.einsum(
        "oyx,ioyx->iyx", grad_real, weight_imag, precision=precise
    )
    return jnp.stack([back_real, back_imag], axis=2)


def outer_grad(spectra, grads):
    spec_real = spectra[:, :, 0]
    spec_imag = spectra[:, :, 1]
    grad_real = grads[:, :, 0]
    grad_imag = grads[:, :, 1]
    real_side = jnp.einsum("iyx,oyx->ioyx", spec_real, grad_real) + jnp.einsum(
        "iyx,oyx->ioyx", spec_imag, grad_imag
    )
    imag_side = jnp.einsum("iyx,oyx->ioyx", spec_real, grad_imag) - jnp.einsum(
        "iyx,oyx->ioyx", spec_imag, grad_real
    )
    return jnp.stack([real_side, imag_side], axis=3)


def mode_weights(limit_rows, col_freq, row_freq, kx_count, cells_total):
    keep_cols = col_freq[None, :] < limit_rows[:, 0:1]
    keep_rows = (row_freq[None, :] < limit_rows[:, 1:2]) | (
        (kx_count - row_freq)[None, :] < limit_rows[:, 1:2]
    )
    scales = jnp.where(col_freq == 0, 1.0, 2.0).astype(jnp.float32) / cells_total
    joined = keep_cols[:, :, None] & keep_rows[:, None, :]
    return (joined.astype(jnp.float32) * scales[None, :, None])[:, :, None, :]


def read_mask(in_index, width_limit):
    return (in_index[:, None] < width_limit[None, :]).astype(jnp.float32)[:, :, None, None, None]


def plain_local(
    source_field, cotangent, spectral_weight, skip_gain, channel_bias, mode_limit, width_limit
):
    channels, row_count, col_count = source_field.shape
    slab_count = lax.axis_size("slab")
    mode_count = lax.axis_size("mode")
    slab_index = lax.axis_index("slab")
    mode_index = lax.axis_index("mode")
    chan_index = lax.axis_index("chan")
    local_freq = spectral_weight.shape[2]
    local_kx = spectral_weight.shape[4]
    freq_count = local_freq * mode_count
    kx_count = local_kx * slab_count
    all_rows = row_count * slab_count
    all_cols = col_count * mode_count
    column_tab = column_table(all_cols, freq_count, mode_index * col_count, col_count)
    row_cos, row_sin = row_tables(all_rows, freq_count, slab_index * row_count, row_count)

    def spectrum(values):
        partial_cols = jnp.einsum("chw,wk->ckh", values, column_tab, precision=precise)
        summed_cols = lax.psum_scatter(partial_cols, "mode", scatter_dimension=1, tiled=True)
        paired = summed_cols.reshape(values.shape[0] * local_freq, 2, row_count)
        spectra = lax.psum_scatter(
            row_forward(paired, row_cos, row_sin), "slab", scatter_dimension=2, tiled=True
        )
        return spectra.reshape(values.shape[0], local_freq, 2, local_kx)

    def synthesis(modes_in):
        whole_modes = lax.all_gather(modes_in, "slab", axis=3, tiled=True)
        rebuilt = row_inverse(
            whole_modes.reshape(channels * local_freq, 2, kx_count), row_cos, row_sin
        )
        rebuilt = rebuilt.reshape(channels, 2 * local_freq, row_count)
        gathered = lax.all_gather(rebuilt, "mode", axis=1, tiled=True)
        return jnp.einsum("ckh,wk->chw", gathered, column_tab, precision=precise)

    in_index = chan_index * channels + jnp.arange(channels, dtype=jnp.int32)
    col_freq = mode_index * local_freq + jnp.arange(local_freq, dtype=jnp.int32)
    row_freq = slab_index * local_kx + jnp.arange(local_kx, dtype=jnp.int32)
    limit_rows = lax.dynamic_slice_in_dim(mode_limit, chan_index * channels, channels, 0)
    weights = mode_weights(limit_rows, col_freq, row_freq, kx_count, all_rows * all_cols)
    reads = read_mask(in_index, width_limit)
    masked_weight = spectral_weight * reads
    spectra = spectrum(source_field)
    out_modes = (
        lax.psum_scatter(contract(spectra, masked_weight), "chan", scatter_dimension=0, tiled=True)
        * weights
    )
    branch = synthesis(out_modes)
    skip_scale = skip_gain[:, None, None]
    summed = branch + skip_scale * source_field + channel_bias[:, None, None]
    output, gelu_back = jax.vjp(jax.nn.gelu, summed)
    grad_sum = gelu_back(cotangent)[0]
    grad_modes = spectrum(grad_sum) * weights
    all_grads = lax.all_gather(grad_modes, "chan", axis=0, tiled=True)
    spectral_grad = outer_grad(spectra, all_grads) * reads
    field_grad = synthesis(contract_back(all_grads, masked_weight)) + skip_scale * grad_sum
    gate_grad, bias_grad = lax.psum(
        (jnp.sum(grad_sum * source_field, axis=(1, 2)), jnp.sum(grad_sum, axis=(1, 2))),
        ("slab", "mode"),
    )
    return (output, field_grad, spectral_grad, gate_grad, bias_grad)


def local(*args):
    geo = Geometry(args[0], args[2])
    if geo.fits():
        return fast_local(*args, geo)
    return plain_local(*args)


def solution(mesh):
    in_specs = (
        P(("member", "chan"), "slab", "mode"),
        P(("member", "chan"), "slab", "mode"),
        P(("member", "chan"), None, "mode", None, "slab"),
        P(("member", "chan")),
        P(("member", "chan")),
        P("member", None),
        P("member"),
    )
    out_specs = (
        P(("member", "chan"), "slab", "mode"),
        P(("member", "chan"), "slab", "mode"),
        P(("member", "chan"), None, "mode", None, "slab"),
        P(("member", "chan")),
        P(("member", "chan")),
    )
    return jax.shard_map(local, mesh=mesh, in_specs=in_specs, out_specs=out_specs, check_vma=False)
```

```python
import functools
import math

import jax
import jax.numpy as jnp
from jax import lax
from jax.experimental import pallas as pl
from jax.experimental.pallas import tpu as pltpu
from jax.sharding import PartitionSpec as P

F32 = jnp.float32
BF16 = jnp.bfloat16
LANES = 128
GELU_A = math.sqrt(2.0 / math.pi)
GELU_B = GELU_A * 0.044715


def split(x):
    high = x.astype(BF16)
    return high, (x - high.astype(F32)).astype(BF16)


def split_table(x):
    high = lax.reduce_precision(x, 8, 7)
    return high.astype(BF16), (x - high).astype(BF16)


def mm(a, b):
    return jnp.dot(a, b, preferred_element_type=F32)


def angles(cells, freqs, extent):
    products = (cells[:, None] * freqs[None, :] % extent).astype(F32)
    return products * (2.0 * math.pi / extent)


def plan_tables(geo):
    col_cell = geo.mode * geo.cols + jnp.arange(geo.cols, dtype=jnp.int32)
    rel_mode = (geo.mode + jnp.arange(geo.modes, dtype=jnp.int32)) % geo.modes
    freq = (rel_mode[:, None] * geo.freq + jnp.arange(geo.freq, dtype=jnp.int32)[None, :])
    theta = angles(col_cell, freq.reshape(-1), geo.all_cols).reshape(geo.cols, geo.modes, geo.freq)
    cos, sin = jnp.cos(theta), jnp.sin(theta)
    first = jnp.stack([cos, -sin], axis=2).reshape(geo.cols, -1)
    second = jnp.stack([-sin, -cos], axis=2).reshape(geo.cols, -1)
    first_h, first_l = split_table(first)
    second_h, second_l = split_table(second)
    forward_cols = jnp.concatenate([first_h, first_l], axis=1)
    inverse_cols = jnp.stack(
        [
            jnp.concatenate([high.T, high.T, low.T, low.T], axis=0)
            for high, low in ((first_h, first_l), (second_h, second_l))
        ]
    )
    row_cell = geo.slab * geo.rows + jnp.arange(geo.rows, dtype=jnp.int32)
    rel_slab = (geo.slab + jnp.arange(geo.slabs, dtype=jnp.int32)) % geo.slabs
    place = (rel_slab[:, None] * geo.kx + jnp.arange(geo.kx, dtype=jnp.int32)[None, :]).reshape(-1)
    half = geo.slabs * geo.kx // 2
    wave = jnp.where(place < half, place, place - 2 * half)
    theta = angles(wave % geo.all_rows, row_cell, geo.all_rows)
    forward_h, forward_l = split_table(jnp.concatenate([jnp.cos(theta), jnp.sin(theta)], axis=0))
    forward_rows = jnp.concatenate([forward_h, forward_l], axis=0)
    kept = jnp.arange(geo.fold // 2, dtype=jnp.int32)
    theta = angles(row_cell, kept, geo.all_rows)
    live = (kept <= half)[None, :]
    inverse_h, inverse_l = split_table(
        jnp.concatenate(
            [jnp.where(live, jnp.cos(theta), 0.0), jnp.where(live, jnp.sin(theta), 0.0)], axis=1
        )
    )
    rest = jnp.zeros((geo.rows, 256 - 3 * geo.fold), BF16)
    inverse_rows = jnp.concatenate([inverse_h, inverse_h, inverse_l, rest], axis=1)
    same = (jnp.abs(wave)[None, :] == kept[:, None]).astype(F32)
    fold = jnp.concatenate([same, same * jnp.sign(wave).astype(F32)[None, :]], axis=0).astype(BF16)
    return forward_cols, forward_rows, inverse_cols, inverse_rows, jnp.concatenate([fold, fold], axis=1)


def lane_group(shape, width):
    return lax.broadcasted_iota(jnp.int32, shape, 1) // width


def pair_spectra(first, second, row_tab, freq):
    sides = row_tab.shape[0] // 2
    high, low = split(jnp.concatenate([first, second], axis=1))
    both = mm(row_tab, high)
    total = both[:sides] + both[sides:] + mm(row_tab[:sides], low)
    out = []
    for lane in (0, LANES):
        one = total[:, lane : lane + LANES]
        one = one + pltpu.roll(one, 64, 1)
        cos, sin = one[: sides // 2], one[sides // 2 :]
        real = lane_group(sin.shape, freq) % 2 == 0
        out.append(cos + jnp.where(real, pltpu.roll(sin, LANES - freq, 1), -pltpu.roll(sin, freq, 1)))
    return out


def write_spectra(doubled, own_ref, other_ref, group):
    turned = [pltpu.roll(s, 32, 1) for s in doubled]
    place = lane_group(doubled[0].shape, 32)

    def weave(arrays):
        return jnp.where(
            place == 0,
            arrays[0],
            jnp.where(place == 1, arrays[1], jnp.where(place == 2, arrays[2], arrays[3])),
        )

    own = weave([doubled[0], turned[1], doubled[2], turned[3]])
    other = weave([turned[0], doubled[1], turned[2], doubled[3]])
    slabs, _, kx, _ = own_ref.shape
    for q in range(slabs):
        own_ref[q, group] = own[q * kx : (q + 1) * kx]
        other_ref[q, group] = other[q * kx : (q + 1) * kx]


def emitting(part_ref, row_ref, own_ref, other_ref, at, freq):
    held = {}

    def pair(k):
        held[k] = pair_spectra(part_ref[2 * k], part_ref[2 * k + 1], row_ref[...], freq)

    def write():
        write_spectra(held[0] + held[1], own_ref, other_ref, at)

    return [functools.partial(pair, 0), functools.partial(pair, 1), write]


def forward_kernel(place_ref, x_ref, col_ref, row_ref, own_ref, other_ref, keep_ref, sems, part_ref, *, freq):
    del place_ref
    step = pl.program_id(0)

    def fetching(at):
        four = pl.ds(at * 4, 4)
        return pltpu.make_async_copy(x_ref.at[four], keep_ref.at[four], sems.at[at])

    @pl.when(step == 0)
    def _():
        for at in range(FORWARD_AHEAD):
            fetching(at).start()

    @pl.when(step + FORWARD_AHEAD < pl.num_programs(0))
    def _():
        fetching(step + FORWARD_AHEAD).start()

    @pl.when(step == 0)
    def _():
        part_ref[...] = jnp.zeros_like(part_ref)

    fetching(step).wait()
    emits = emitting(part_ref, row_ref, own_ref, other_ref, jnp.maximum(step - 1, 0), freq)
    for c in range(4):
        if c < len(emits):
            emits[c]()
        high, low = split(keep_ref[step * 4 + c])
        part_ref[c] = mm(high, col_ref[...]) + mm(low, col_ref[...])

    @pl.when(step == pl.num_programs(0) - 1)
    def _():
        for task in emitting(part_ref, row_ref, own_ref, other_ref, step, freq):
            task()


def fold_modes(piece_refs, step, fold_ref):
    slabs = len(piece_refs) // 2
    halves = [
        jnp.concatenate([r[step] for r in piece_refs[m * slabs : (m + 1) * slabs]], axis=0) for m in (0, 1)
    ]
    high, low = split(jnp.concatenate(halves, axis=1))
    return mm(fold_ref[...], jnp.concatenate([high, low], axis=0))


def line_up(folded, c):
    group = lane_group((folded.shape[0], LANES), 32)
    a, b = folded[:, :LANES], folded[:, LANES:]
    a_at = [a if (t - c) % 4 == 0 else pltpu.roll(a, 32 * ((t - c) % 4), 1) for t in (0, 2)]
    b_at = [b if (t - c) % 4 == 0 else pltpu.roll(b, 32 * ((t - c) % 4), 1) for t in (1, 3)]
    one = jnp.where(
        group == 0, a_at[0], jnp.where(group == 1, b_at[0], jnp.where(group == 2, a_at[1], b_at[1]))
    )
    top = one.astype(BF16).astype(F32)
    return jnp.where(group < 2, top, one - top)


def spread_columns(rows, side, inv_col_ref):
    half = rows[0].shape[0] // 2
    lhs = jnp.concatenate([r[side * half : (side + 1) * half] for r in rows], axis=0).astype(BF16)
    return mm(jnp.concatenate([lhs, lhs], axis=1), inv_col_ref[side])


def stack_operand(plus, minus, add=None):
    if add is not None:
        plus = plus + jnp.where(lax.broadcasted_iota(jnp.int32, plus.shape, 0) == 0, add, 0.0)
    high, low = split(jnp.concatenate([plus, minus], axis=0))
    rest = jnp.zeros((256 - 3 * high.shape[0], high.shape[1]), BF16)
    return jnp.concatenate([high, low, high, rest], axis=0)


def preparing(piece_refs, at, fold_ref, inv_col_ref, wide_ref, ready, biases):
    held = {}
    half = fold_ref.shape[0] // 2

    def begin():
        held["folded"] = fold_modes(piece_refs, at, fold_ref)

    def line(c):
        held[c] = line_up(held["folded"], c)

    def spread(side):
        wide_ref[side] = spread_columns([held[c] for c in range(4)], side, inv_col_ref)

    def stack(c):
        plus, minus = (wide_ref[side, c * half : (c + 1) * half] for side in (0, 1))
        ready[c] = stack_operand(plus, minus, None if biases is None else biases[c])

    early = [begin] + [functools.partial(line, c) for c in range(4)]
    early += [functools.partial(spread, side) for side in (0, 1)]
    return early, [functools.partial(stack, c) for c in range(4)]


CHUNK = 16


def middle_kernel(place_ref, skip_ref, bias_ref, *refs, pieces, freq):
    piece_refs = refs[:pieces]
    x_ref, ct_ref, fold_ref, inv_col_ref, inv_row_ref, col_ref, row_ref = refs[pieces : pieces + 7]
    out_ref, gs_ref, own_ref, other_ref, ready, wide_ref, branch, high_ref, low_ref, part_ref = refs[pieces + 7 :]
    step = pl.program_id(0)
    last = pl.num_programs(0) - 1
    rows, cols = x_ref.shape[1:]
    sums = own_ref.shape[1] - 1

    def prepare_group(at):
        biases = [bias_ref[at * 4 + c] for c in range(4)]
        return preparing(piece_refs, at, fold_ref, inv_col_ref, wide_ref, ready, biases)

    def transform(c):
        part_ref[c] = mm(high_ref[c], col_ref[...]) + mm(low_ref[c], col_ref[...])

    def emit_group(at):
        return emitting(part_ref, row_ref, own_ref, other_ref, at, freq)

    @pl.when(step == 0)
    def _():
        early, late = prepare_group(0)
        for task in early + late:
            task()
        part_ref[...] = jnp.zeros_like(part_ref)
        high_ref[3] = jnp.zeros_like(high_ref[3])
        low_ref[3] = jnp.zeros_like(low_ref[3])
        own_ref[0, sums] = jnp.zeros(own_ref.shape[2:], F32)

    early, late = prepare_group(jnp.minimum(step + 1, last))
    emits = emit_group(jnp.maximum(step - 1, 0))
    chunks = rows // CHUNK
    plan = {(0, 2): emits[0], (0, 6): emits[1], (0, 11): emits[2]}
    for k, task in enumerate(early):
        plan[(1 + k // 4, 2 + 3 * (k % 4))] = task
    for k, task in enumerate(late):
        plan[(3, 2 + 3 * k)] = task
    tile = own_ref[0, sums]
    row = lax.broadcasted_iota(jnp.int32, tile.shape, 0)
    lane = lax.broadcasted_iota(jnp.int32, tile.shape, 1)
    branch[0] = mm(inv_row_ref[...], ready[0])
    for c in range(4):
        channel = step * 4 + c
        skip = skip_ref[channel]
        gate = jnp.zeros((CHUNK, cols), F32)
        for k in range(chunks):
            r = k * CHUNK
            if (c, k) in plan:
                plan[(c, k)]()
            if k == 0 and c < 3:
                branch[c + 1] = mm(inv_row_ref[...], ready[c + 1])
            if k == 1 and c > 0:
                transform(c - 1)
            if k == 0 and c == 0:
                transform(3)
            x = x_ref[channel, r : r + CHUNK]
            v = branch[c, r : r + CHUNK] + skip * x
            q = v * v
            t = jnp.tanh(v * (q * GELU_B + GELU_A))
            s = 0.5 * t + 0.5
            out = v * s
            out_ref[c, r : r + CHUNK] = out
            slope = s + out * (1.0 - s) * (q * (6.0 * GELU_B) + 2.0 * GELU_A)
            grad = ct_ref[c, r : r + CHUNK] * slope
            gs_ref[channel, r : r + CHUNK] = grad
            gate = gate + grad * x
            top = grad.astype(BF16)
            high_ref[c, r : r + CHUNK] = top
            low_ref[c, r : r + CHUNK] = (grad - top.astype(F32)).astype(BF16)
        line = jnp.sum(gate, axis=0, keepdims=True)
        value = jnp.sum(sum(line[:, k : k + LANES] for k in range(0, cols, LANES)), axis=1, keepdims=True)
        tile = jnp.where((row == 0) & (lane == channel), jnp.broadcast_to(value, tile.shape), tile)
    own_ref[0, sums] = tile

    @pl.when(step == last)
    def _():
        transform(3)
        for task in emit_group(last):
            task()
        whole_sums = tile
        for g in range(sums):
            lines = [ref[place_ref[4], g][0:1, :] for ref in (own_ref, other_ref)]
            line = jnp.where(place_ref[0] == 0, lines[0], lines[1])
            for c in range(4):
                value = jnp.broadcast_to(line[:, 2 * freq * c : 2 * freq * c + 1], tile.shape)
                whole_sums = jnp.where((row == 1) & (lane == g * 4 + c), value, whole_sums)
        for q in range(own_ref.shape[0]):
            own_ref[q, sums] = whole_sums
            other_ref[q, sums] = whole_sums


def last_kernel(skip_ref, *refs, pieces):
    piece_refs = refs[:pieces]
    gs_ref, fold_ref, inv_col_ref, inv_row_ref, out_ref, made_ref, sems, ready, wide_ref = refs[pieces:]
    step = pl.program_id(0)
    last = pl.num_programs(0) - 1

    def storing(at):
        four = pl.ds(at * 4, 4)
        return pltpu.make_async_copy(made_ref.at[four], out_ref.at[four], sems.at[at])

    def prepare_group(at):
        return preparing(piece_refs, at, fold_ref, inv_col_ref, wide_ref, ready, None)

    @pl.when(step == 0)
    def _():
        early, late = prepare_group(0)
        for task in early + late:
            task()

    early, late = prepare_group(jnp.minimum(step + 1, last))
    turns = [early[:1], early[1:5], early[5:], []]
    for c in range(4):
        channel = step * 4 + c
        made_ref[channel] = mm(inv_row_ref[...], ready[c]) + skip_ref[channel] * gs_ref[channel]
        for task in turns[c]:
            task()
    for task in late:
        task()
    storing(step).start()

    @pl.when(step == last)
    def _():
        for at in range(sems.shape[0]):
            storing(at).wait()


def limits_mask(place_ref, limit_ref, y, kx, kx_all, scale_cells, shape):
    col = place_ref[0] + y
    row = place_ref[1] + lax.broadcasted_iota(jnp.int32, shape, 0)
    wide = jnp.broadcast_to(limit_ref[0:1, :], shape)
    tall = jnp.broadcast_to(limit_ref[1:2, :], shape)
    keep = (col < wide) & ((row < tall) | (kx_all - row < tall))
    scale = jnp.where(col == 0, 1.0 / scale_cells, 2.0 / scale_cells).astype(F32)
    return jnp.where(keep, scale, 0.0)


def pick_table(geo):
    source = lax.broadcasted_iota(jnp.int32, (2 * LANES, 8 * LANES), 0) % LANES
    target = lax.broadcasted_iota(jnp.int32, (2 * LANES, 8 * LANES), 1) // LANES
    return (source == target * geo.freq).astype(BF16)


def spread_lanes(spec, y, pick_ref):
    turned = pltpu.roll(spec, LANES - y, 1)
    high, low = split(turned)
    lhs = jnp.concatenate([high, low], axis=1)
    return [mm(lhs, pick_ref[:, 2 * LANES * c : 2 * LANES * (c + 1)]) for c in range(4)]


def mix_kernel(
    place_ref, r0, r1, r2, r3, w_ref, limit_ref, width_ref, pick_ref, held_ref, mine_ref, theirs_ref, spec_ref, made, turn, laid, *, geo, block
):
    freq, kx, outs = geo.freq, geo.kx, geo.outs
    groups = spec_ref.shape[0]
    step = pl.program_id(0)
    half = groups * kx

    @pl.when(step == 0)
    def _():
        spec_ref[...] = r0[...] + r1[...] + r2[...] + r3[...]

    widths = width_ref[0:1, :] - place_ref[2]
    spec = spec_ref[...].reshape(half, LANES)
    for k in range(block):
        y = step * block + k
        re = jnp.zeros((kx, outs), F32)
        im = jnp.zeros((kx, outs), F32)
        spread = spread_lanes(spec, y, pick_ref)
        for c in range(4):
            for g in range(groups):
                i = g * 4 + c
                sr = spread[c][g * kx : (g + 1) * kx, :outs]
                si = spread[c][g * kx : (g + 1) * kx, LANES : LANES + outs]
                reads = jnp.broadcast_to(widths > i, (kx, outs))
                wr = jnp.where(reads, w_ref[i, y, 0], 0.0)
                wi = jnp.where(reads, w_ref[i, y, 1], 0.0)
                re = re + (sr * wr - si * wi)
                im = im + (sr * wi + si * wr)
        mask = limits_mask(place_ref, limit_ref, y, kx, geo.kx_all, geo.cells, (kx, outs))
        made[pl.ds(y * kx, kx), :outs] = re * mask
        made[pl.ds((freq + y) * kx, kx), :outs] = im * mask

    @pl.when(step == pl.num_programs(0) - 1)
    def _():
        place = lane_group((2 * groups, LANES), 2 * freq)
        for j in range(kx):
            slot = j % turn.shape[0]
            turn[slot, :, : 2 * freq] = made[pl.ds(j, 2 * freq, stride=kx), :].T
            line = jnp.zeros((2 * groups, LANES), F32)
            for c in range(4):
                one = turn[slot, pl.ds(c, 2 * groups, stride=4), :]
                line = jnp.where(place == c, pltpu.roll(one, 2 * freq * c, 1) if c else one, line)
            laid[pl.ds(j, 2 * groups, stride=kx), :] = line
        mine_ref[...] = laid[pl.ds(place_ref[3] * half, half), :].reshape(mine_ref.shape)
        theirs_ref[...] = laid[pl.ds((1 - place_ref[3]) * half, half), :].reshape(mine_ref.shape)


def back_kernel(place_ref, own_ref, peer_ref, w_ref, limit_ref, width_ref, held_ref, out_ref, gm_ref, made, turn, laid, *, geo, block):
    freq, kx, outs = geo.freq, geo.kx, geo.outs
    step = pl.program_id(0)
    groups = out_ref.shape[0]
    half = groups * kx
    lane = lax.broadcasted_iota(jnp.int32, (kx, LANES), 1)

    @pl.when(step == 0)
    def _():
        laid[pl.ds(place_ref[3] * half, half), :] = own_ref[...].reshape(half, LANES)
        laid[pl.ds((1 - place_ref[3]) * half, half), :] = peer_ref[...].reshape(half, LANES)
        for j in range(kx):
            slot = j % turn.shape[0]
            line = laid[pl.ds(j, 2 * groups, stride=kx), :]
            for c in range(4):
                turn[slot, pl.ds(c, 2 * groups, stride=4), :] = (
                    pltpu.roll(line, LANES - 2 * freq * c, 1) if c else line
                )
            made[pl.ds(j, 2 * freq, stride=kx), :] = turn[slot].T[: 2 * freq]
        out_ref[...] = jnp.zeros_like(out_ref)

    widths = width_ref[0:1, :] - place_ref[2]
    for k in range(block):
        y = step * block + k
        mask = limits_mask(place_ref, limit_ref, y, kx, geo.kx_all, geo.cells, (kx, outs))
        gr = made[pl.ds(y * kx, kx), :outs] * mask
        gi = made[pl.ds((freq + y) * kx, kx), :outs] * mask
        gm_ref[k, 0] = gr
        gm_ref[k, 1] = gi
        for g in range(groups):
            line = out_ref[g]
            for c in range(4):
                i = g * 4 + c
                reads = jnp.broadcast_to(widths > i, (kx, outs))
                wr = jnp.where(reads, w_ref[i, y, 0], 0.0)
                wi = jnp.where(reads, w_ref[i, y, 1], 0.0)
                br = jnp.sum(gr * wr + gi * wi, axis=1, keepdims=True)
                bi = jnp.sum(gi * wr - gr * wi, axis=1, keepdims=True)
                line = jnp.where(lane == 32 * c + y, jnp.broadcast_to(br, (kx, LANES)), line)
                line = jnp.where(lane == 32 * c + freq + y, jnp.broadcast_to(bi, (kx, LANES)), line)
            out_ref[g] = line


def outer_kernel(place_ref, spec_ref, gm_ref, width_ref, pick_ref, held_ref, out_ref, *, geo):
    kx, outs = geo.kx, geo.outs
    block = out_ref.shape[1]
    step = pl.program_id(0)
    groups = spec_ref.shape[0]
    widths = width_ref[0:1, :] - place_ref[2]
    spec = spec_ref[...].reshape(groups * kx, LANES)
    for k in range(block):
        gr = gm_ref[k, 0]
        gi = gm_ref[k, 1]
        spread = spread_lanes(spec, step * block + k, pick_ref)
        for c in range(4):
            for g in range(groups):
                i = g * 4 + c
                sr = spread[c][g * kx : (g + 1) * kx, :outs]
                si = spread[c][g * kx : (g + 1) * kx, LANES : LANES + outs]
                reads = jnp.broadcast_to(widths > i, (kx, outs))
                out_ref[i, k, 0] = jnp.where(reads, sr * gr + si * gi, 0.0)
                out_ref[i, k, 1] = jnp.where(reads, sr * gi - si * gr, 0.0)


def prefetch_kernel(after_ref, held_ref, source_ref, target_ref, sem):
    del after_ref, held_ref
    copy = pltpu.make_async_copy(source_ref, target_ref, sem)
    copy.start()
    copy.wait()


def prefetch(x, after, held):
    anywhere = pl.BlockSpec(memory_space=pl.ANY)
    return pl.pallas_call(
        prefetch_kernel,
        in_specs=[anywhere] * 3,
        out_specs=anywhere,
        out_shape=pltpu.VMEM(x.shape, x.dtype),
        scratch_shapes=[pltpu.SemaphoreType.DMA],
        compiler_params=pltpu.CompilerParams(vmem_limit_bytes=1 << 20),
        cost_estimate=cost(4),
        name="prefetch",
    )(after, resident(held), streamed(x))


class Geometry:
    def __init__(self, field, weight):
        self.channels, self.rows, self.cols = field.shape
        self.outs, self.freq, self.kx = weight.shape[1], weight.shape[2], weight.shape[4]
        self.slabs = lax.axis_size("slab")
        self.modes = lax.axis_size("mode")
        self.chans = lax.axis_size("chan")
        self.slab = lax.axis_index("slab")
        self.mode = lax.axis_index("mode")
        self.chan = lax.axis_index("chan")
        self.kx_all = self.kx * self.slabs
        self.all_rows = self.rows * self.slabs
        self.all_cols = self.cols * self.modes
        self.cells = float(self.all_rows * self.all_cols)
        self.fold = 16 * ((2 * (self.kx_all // 2 + 1) + 15) // 16)

    def fits(self):
        return (
            self.modes == 2
            and self.chans == 2
            and self.slabs == 4
            and self.freq == 16
            and self.kx_all == 64
            and self.kx % 8 == 0
            and self.channels % 4 == 0
            and self.channels <= LANES
            and self.rows % 16 == 0
            and self.cols % LANES == 0
            and 3 * self.fold <= 256
        )


def swap(x, name):
    n = lax.axis_size(name)
    return lax.ppermute(x, name, [(i, (i + 1) % n) for i in range(n)])


def fetch(x, name, distance):
    n = lax.axis_size(name)
    return lax.ppermute(x, name, [((i + distance) % n, i) for i in range(n)])


def send(x, name, distance):
    n = lax.axis_size(name)
    return lax.ppermute(x, name, [(i, (i + distance) % n) for i in range(n)])


def whole(shape):
    return pl.BlockSpec(shape, lambda *_: (0,) * len(shape))


SMEM = pl.BlockSpec(memory_space=pltpu.SMEM)


FORWARD_LIMIT = 16 << 20
FORWARD_AHEAD = 3
MIX_LIMIT = 16 << 20
MIDDLE_LIMIT = 24 << 20
LAST_LIMIT = 28 << 20


def cost(micros):
    return pl.CostEstimate(flops=int(micros * 1.0e8), bytes_accessed=1 << 20, transcendentals=0)


def params(limit):
    return pltpu.CompilerParams(dimension_semantics=("arbitrary",), vmem_limit_bytes=limit)


VMEM = pl.BlockSpec(memory_space=pltpu.VMEM)
ANYWHERE = pl.BlockSpec(memory_space=pl.ANY)


def streamed(x):
    return pltpu.with_memory_space_constraint(x, pltpu.HBM)


def resident(x):
    return pltpu.with_memory_space_constraint(x, pltpu.VMEM)


def reduce_spectrum(own, other, geo):
    own = own + swap(other, "mode")
    return [own[0]] + [send(own[d], "slab", d) for d in range(1, geo.slabs)]


def gather_slabs(mine, geo):
    return [mine] + [fetch(mine, "slab", d) for d in range(1, geo.slabs)]


def gather_halves(near):
    return near + [swap(piece, "mode") for piece in near]


def fast_local(
    source_field, cotangent, spectral_weight, skip_gain, channel_bias, mode_limit, width_limit, geo
):
    channels, rows, cols = source_field.shape
    groups = channels // 4
    fwd_cols, fwd_rows, inv_cols, inv_rows, fold = plan_tables(geo)
    pick = pick_table(geo)
    weight = jnp.transpose(spectral_weight, (0, 2, 3, 4, 1))
    field = source_field.shape
    field_spec = pl.BlockSpec((4, rows, cols), lambda s: (s, 0, 0))
    piece = (groups, geo.kx, LANES)
    piece_shape = jax.ShapeDtypeStruct(piece, F32)
    place = jnp.stack([geo.mode * geo.freq, geo.slab * geo.kx, geo.chan * channels, geo.chan, -geo.slab % geo.slabs]).astype(jnp.int32)
    limits = jnp.transpose(mode_limit)
    widths = width_limit[None, :]

    own, other, kept = pl.pallas_call(
        functools.partial(forward_kernel, freq=geo.freq),
        grid=(groups,),
        in_specs=[SMEM, ANYWHERE, VMEM, VMEM],
        out_specs=[VMEM] * 3,
        out_shape=[jax.ShapeDtypeStruct((geo.slabs,) + piece, F32)] * 2 + [pltpu.VMEM(field, F32)],
        scratch_shapes=[pltpu.SemaphoreType.DMA((groups,)), pltpu.VMEM((4, rows, LANES), F32)],
        compiler_params=params(FORWARD_LIMIT),
        cost_estimate=cost(6),
        name="forward",
    )(place, streamed(source_field), fwd_cols, fwd_rows)
    parts = reduce_spectrum(own, other, geo)
    near_weight = prefetch(weight, parts[0], kept)

    block = 4
    steps = geo.freq // block
    w_out = pl.BlockSpec((channels, block, 2, geo.kx, geo.outs), lambda s: (0, s, 0, 0, 0))
    g_spec = pl.BlockSpec((block, 2, geo.kx, geo.outs), lambda s: (s, 0, 0, 0))
    modes_shape = jax.ShapeDtypeStruct((geo.freq, 2, geo.kx, geo.outs), F32)
    relay = [
        pltpu.VMEM((2 * geo.freq * geo.kx, LANES), F32),
        pltpu.VMEM((4, LANES, LANES), F32),
        pltpu.VMEM((2 * groups * geo.kx, LANES), F32),
    ]
    mine, theirs, spectra = pl.pallas_call(
        functools.partial(mix_kernel, geo=geo, block=block),
        grid=(steps,),
        in_specs=[SMEM] + [VMEM] * 8 + [ANYWHERE],
        out_specs=[VMEM] * 3,
        out_shape=[piece_shape] * 3,
        scratch_shapes=relay,
        compiler_params=params(MIX_LIMIT),
        cost_estimate=cost(3),
        name="mix",
    )(place, *parts, resident(near_weight), limits, widths, pick, resident(kept))
    pieces = gather_halves(gather_slabs(mine + swap(theirs, "chan"), geo))

    wide = jax.ShapeDtypeStruct((geo.slabs, groups + 1) + piece[1:], F32)
    fields = len(pieces) + 3
    output, grad_sum, own, other = pl.pallas_call(
        functools.partial(middle_kernel, pieces=len(pieces), freq=geo.freq),
        grid=(groups,),
        in_specs=[SMEM] * 3 + [VMEM] * (len(pieces) + 1) + [field_spec] + [VMEM] * 5,
        out_specs=[field_spec, VMEM, VMEM, VMEM],
        out_shape=[jax.ShapeDtypeStruct(field, F32), pltpu.VMEM(field, F32), wide, wide],
        scratch_shapes=[
            pltpu.VMEM((4, 256, cols), BF16),
            pltpu.VMEM((2, 2 * geo.fold, cols), F32),
            pltpu.VMEM((4, rows, cols), F32),
            pltpu.VMEM((4, rows, cols), BF16),
            pltpu.VMEM((4, rows, cols), BF16),
            pltpu.VMEM((4, rows, LANES), F32),
        ],
        input_output_aliases={fields: 1},
        compiler_params=params(MIDDLE_LIMIT),
        cost_estimate=cost(20),
        name="middle",
    )(
        place, skip_gain, channel_bias, *pieces, resident(kept), streamed(cotangent), fold, inv_cols, inv_rows, fwd_cols, fwd_rows
    )
    parts = reduce_spectrum(own, other, geo)
    near_weight = prefetch(weight, parts[0], grad_sum)
    parts, near_weight = lax.optimization_barrier((parts, near_weight))
    grads = parts[0] + parts[1] + parts[2] + parts[3]
    sums = grads[groups]
    grads = grads[:groups]
    back, grad_modes = pl.pallas_call(
        functools.partial(back_kernel, geo=geo, block=block),
        grid=(steps,),
        in_specs=[SMEM] + [VMEM] * 5 + [ANYWHERE],
        out_specs=[VMEM, g_spec],
        out_shape=[piece_shape, modes_shape],
        scratch_shapes=relay,
        compiler_params=params(MIX_LIMIT),
        cost_estimate=cost(3),
        name="back",
    )(place, grads, swap(grads, "chan"), resident(near_weight), limits, widths, resident(grad_sum))
    near = gather_slabs(back, geo)
    spectral_grad = pl.pallas_call(
        functools.partial(outer_kernel, geo=geo),
        grid=(steps,),
        in_specs=[SMEM, VMEM, g_spec, VMEM, VMEM, ANYWHERE],
        out_specs=w_out,
        out_shape=jax.ShapeDtypeStruct(weight.shape, F32),
        compiler_params=params(MIX_LIMIT),
        cost_estimate=cost(4),
        name="outer",
    )(place, spectra, grad_modes, widths, pick, resident(grad_sum))
    near, spectral_grad = lax.optimization_barrier((near, spectral_grad))
    pieces = gather_halves(near)
    field_grad = pl.pallas_call(
        functools.partial(last_kernel, pieces=len(pieces)),
        grid=(groups,),
        in_specs=[SMEM] + [VMEM] * (len(pieces) + 4),
        out_specs=ANYWHERE,
        out_shape=jax.ShapeDtypeStruct(field, F32),
        scratch_shapes=[
            pltpu.VMEM(field, F32),
            pltpu.SemaphoreType.DMA((groups,)),
            pltpu.VMEM((4, 256, cols), BF16),
            pltpu.VMEM((2, 2 * geo.fold, cols), F32),
        ],
        compiler_params=params(LAST_LIMIT),
        cost_estimate=cost(7),
        name="last",
    )(skip_gain, *pieces, resident(grad_sum), fold, inv_cols, inv_rows)
    return (
        output,
        field_grad,
        jnp.transpose(spectral_grad, (0, 4, 1, 2, 3)),
        sums[0, :channels],
        sums[1, :channels],
    )


precise = lax.Precision.HIGHEST


def column_table(extent, freq_count, first_cell, cell_count):
    cell_index = first_cell + jnp.arange(cell_count, dtype=jnp.int32)
    wave_index = jnp.arange(freq_count, dtype=jnp.int32)
    products = (cell_index[:, None] * wave_index[None, :] % extent).astype(jnp.float32)
    angles = products * (2.0 * math.pi / extent)
    return jnp.stack([jnp.cos(angles), -jnp.sin(angles)], axis=-1).reshape(
        cell_count, 2 * freq_count
    )


def row_tables(extent, freq_count, first_cell, cell_count):
    cell_index = first_cell + jnp.arange(cell_count, dtype=jnp.int32)
    column = jnp.arange(2 * freq_count, dtype=jnp.int32)
    wave_index = column + jnp.where(column >= freq_count, extent - 2 * freq_count, 0)
    products = (cell_index[:, None] * wave_index[None, :] % extent).astype(jnp.float32)
    angles = products * (2.0 * math.pi / extent)
    return (jnp.cos(angles), jnp.sin(angles))


def row_forward(lined, row_cos, row_sin):
    line_real = lined[:, 0]
    line_imag = lined[:, 1]
    out_real = jnp.dot(line_real, row_cos, precision=precise) + jnp.dot(
        line_imag, row_sin, precision=precise
    )
    out_imag = jnp.dot(line_imag, row_cos, precision=precise) - jnp.dot(
        line_real, row_sin, precision=precise
    )
    return jnp.stack([out_real, out_imag], axis=1)


def row_inverse(modes_in, row_cos, row_sin):
    mode_real = modes_in[:, 0]
    mode_imag = modes_in[:, 1]
    back_real = jnp.dot(mode_real, row_cos.T, precision=precise) - jnp.dot(
        mode_imag, row_sin.T, precision=precise
    )
    back_imag = jnp.dot(mode_real, row_sin.T, precision=precise) + jnp.dot(
        mode_imag, row_cos.T, precision=precise
    )
    return jnp.stack([back_real, back_imag], axis=1)


def contract(spectra, weight):
    spec_real = spectra[:, :, 0]
    spec_imag = spectra[:, :, 1]
    weight_real = weight[:, :, :, 0]
    weight_imag = weight[:, :, :, 1]
    out_real = jnp.einsum("iyx,ioyx->oyx", spec_real, weight_real, precision=precise) - jnp.einsum(
        "iyx,ioyx->oyx", spec_imag, weight_imag, precision=precise
    )
    out_imag = jnp.einsum("iyx,ioyx->oyx", spec_real, weight_imag, precision=precise) + jnp.einsum(
        "iyx,ioyx->oyx", spec_imag, weight_real, precision=precise
    )
    return jnp.stack([out_real, out_imag], axis=2)


def contract_back(grads, weight):
    grad_real = grads[:, :, 0]
    grad_imag = grads[:, :, 1]
    weight_real = weight[:, :, :, 0]
    weight_imag = weight[:, :, :, 1]
    back_real = jnp.einsum("oyx,ioyx->iyx", grad_real, weight_real, precision=precise) + jnp.einsum(
        "oyx,ioyx->iyx", grad_imag, weight_imag, precision=precise
    )
    back_imag = jnp.einsum("oyx,ioyx->iyx", grad_imag, weight_real, precision=precise) - jnp.einsum(
        "oyx,ioyx->iyx", grad_real, weight_imag, precision=precise
    )
    return jnp.stack([back_real, back_imag], axis=2)


def outer_grad(spectra, grads):
    spec_real = spectra[:, :, 0]
    spec_imag = spectra[:, :, 1]
    grad_real = grads[:, :, 0]
    grad_imag = grads[:, :, 1]
    real_side = jnp.einsum("iyx,oyx->ioyx", spec_real, grad_real) + jnp.einsum(
        "iyx,oyx->ioyx", spec_imag, grad_imag
    )
    imag_side = jnp.einsum("iyx,oyx->ioyx", spec_real, grad_imag) - jnp.einsum(
        "iyx,oyx->ioyx", spec_imag, grad_real
    )
    return jnp.stack([real_side, imag_side], axis=3)


def mode_weights(limit_rows, col_freq, row_freq, kx_count, cells_total):
    keep_cols = col_freq[None, :] < limit_rows[:, 0:1]
    keep_rows = (row_freq[None, :] < limit_rows[:, 1:2]) | (
        (kx_count - row_freq)[None, :] < limit_rows[:, 1:2]
    )
    scales = jnp.where(col_freq == 0, 1.0, 2.0).astype(jnp.float32) / cells_total
    joined = keep_cols[:, :, None] & keep_rows[:, None, :]
    return (joined.astype(jnp.float32) * scales[None, :, None])[:, :, None, :]


def read_mask(in_index, width_limit):
    return (in_index[:, None] < width_limit[None, :]).astype(jnp.float32)[:, :, None, None, None]


def plain_local(
    source_field, cotangent, spectral_weight, skip_gain, channel_bias, mode_limit, width_limit
):
    channels, row_count, col_count = source_field.shape
    slab_count = lax.axis_size("slab")
    mode_count = lax.axis_size("mode")
    slab_index = lax.axis_index("slab")
    mode_index = lax.axis_index("mode")
    chan_index = lax.axis_index("chan")
    local_freq = spectral_weight.shape[2]
    local_kx = spectral_weight.shape[4]
    freq_count = local_freq * mode_count
    kx_count = local_kx * slab_count
    all_rows = row_count * slab_count
    all_cols = col_count * mode_count
    column_tab = column_table(all_cols, freq_count, mode_index * col_count, col_count)
    row_cos, row_sin = row_tables(all_rows, freq_count, slab_index * row_count, row_count)

    def spectrum(values):
        partial_cols = jnp.einsum("chw,wk->ckh", values, column_tab, precision=precise)
        summed_cols = lax.psum_scatter(partial_cols, "mode", scatter_dimension=1, tiled=True)
        paired = summed_cols.reshape(values.shape[0] * local_freq, 2, row_count)
        spectra = lax.psum_scatter(
            row_forward(paired, row_cos, row_sin), "slab", scatter_dimension=2, tiled=True
        )
        return spectra.reshape(values.shape[0], local_freq, 2, local_kx)

    def synthesis(modes_in):
        whole_modes = lax.all_gather(modes_in, "slab", axis=3, tiled=True)
        rebuilt = row_inverse(
            whole_modes.reshape(channels * local_freq, 2, kx_count), row_cos, row_sin
        )
        rebuilt = rebuilt.reshape(channels, 2 * local_freq, row_count)
        gathered = lax.all_gather(rebuilt, "mode", axis=1, tiled=True)
        return jnp.einsum("ckh,wk->chw", gathered, column_tab, precision=precise)

    in_index = chan_index * channels + jnp.arange(channels, dtype=jnp.int32)
    col_freq = mode_index * local_freq + jnp.arange(local_freq, dtype=jnp.int32)
    row_freq = slab_index * local_kx + jnp.arange(local_kx, dtype=jnp.int32)
    limit_rows = lax.dynamic_slice_in_dim(mode_limit, chan_index * channels, channels, 0)
    weights = mode_weights(limit_rows, col_freq, row_freq, kx_count, all_rows * all_cols)
    reads = read_mask(in_index, width_limit)
    masked_weight = spectral_weight * reads
    spectra = spectrum(source_field)
    out_modes = (
        lax.psum_scatter(contract(spectra, masked_weight), "chan", scatter_dimension=0, tiled=True)
        * weights
    )
    branch = synthesis(out_modes)
    skip_scale = skip_gain[:, None, None]
    summed = branch + skip_scale * source_field + channel_bias[:, None, None]
    output, gelu_back = jax.vjp(jax.nn.gelu, summed)
    grad_sum = gelu_back(cotangent)[0]
    grad_modes = spectrum(grad_sum) * weights
    all_grads = lax.all_gather(grad_modes, "chan", axis=0, tiled=True)
    spectral_grad = outer_grad(spectra, all_grads) * reads
    field_grad = synthesis(contract_back(all_grads, masked_weight)) + skip_scale * grad_sum
    gate_grad, bias_grad = lax.psum(
        (jnp.sum(grad_sum * source_field, axis=(1, 2)), jnp.sum(grad_sum, axis=(1, 2))),
        ("slab", "mode"),
    )
    return (output, field_grad, spectral_grad, gate_grad, bias_grad)


def local(*args):
    geo = Geometry(args[0], args[2])
    if geo.fits():
        return fast_local(*args, geo)
    return plain_local(*args)


def solution(mesh):
    in_specs = (
        P(("member", "chan"), "slab", "mode"),
        P(("member", "chan"), "slab", "mode"),
        P(("member", "chan"), None, "mode", None, "slab"),
        P(("member", "chan")),
        P(("member", "chan")),
        P("member", None),
        P("member"),
    )
    out_specs = (
        P(("member", "chan"), "slab", "mode"),
        P(("member", "chan"), "slab", "mode"),
        P(("member", "chan"), None, "mode", None, "slab"),
        P(("member", "chan")),
        P(("member", "chan")),
    )
    return jax.shard_map(local, mesh=mesh, in_specs=in_specs, out_specs=out_specs, check_vma=False)
```
